32 devices in a mesh: groups: 2 (over y), seq: 8 (over z, x), heads: 2 (over core).
Axes of the slice: x: 2, y: 2, z: 4, core: 2. Of those that a mesh axis runs over, the one named last changes fastest.
Arguments:
- queries: bfloat16 [2, 16, 16, 4096], P(None, ('groups', 'seq'), None, 'heads'), parts along dimension 1, may hold values from -8 to 8
- keys: bfloat16 [16, 4096, 512], P(('groups', 'seq'), None, 'heads'), parts along dimension 0, may hold values from -8 to 8
- values: bfloat16 [16, 4096, 512], P(('groups', 'seq'), None, 'heads'), parts along dimension 0, may hold values from -6 to 6
- tile_blocks: int32 [32, 4], P('groups'), parts along dimension 0, may hold values from 0 to 7, all different within a row; in each aligned block of 8 rows (0 to 7, 8 to 15, ...) at most 8 rows name the same one
- block_place: int32 [16], P('groups'), parts along dimension 0, may hold values from 0 to 7, each once
- tile_offset: int32 [32], P('groups'), parts along dimension 0, may hold values from 0 to 255
Outputs:
- attended: bfloat16 [2, 16, 16, 4096], P(None, ('groups', 'seq'), None, 'heads'), parts along dimension 1
The draws below stay inside these ranges and needn't reach their ends.
There are 2 independent parts, one for each index of `groups`. The reference program is written for one: setup_inputs(seed, part) draws one part's arguments, and reference() takes and returns one part's arrays. A program takes and returns all parts, laid end to end along the dimension named above; each array names one. Nothing has to cross between parts.
Inputs may be any that keep to these rules, and one draw needn't show every extreme that they name: `tile_blocks`: each tile lists 4 different blocks; among the 8 tiles of one micro-batch no block is listed by more than 8 tiles, and in some micro-batch one block is listed by exactly 8. `block_place`: each index appears once.
All inputs are finite; a program needn't handle non-finite values.
Results may differ from the reference program's by a relative error of at most 0.0048.
Values may be sent and summed in bfloat16 or wider, within the bound.
No kernel may reach another device: no remote copies, remote signals or barrier semaphores. Data moves between devices by JAX's collectives and lax.ppermute only.
A program may use at most 128 MiB of HBM per device.

```python
import math
import jax
import jax.numpy as jnp
import numpy as np
from jax import lax

HEAD = 128
QHEADS = 32
KV_HEADS = 4
TILE = 16
BLOCK = 4096
TOP = 4
MB = 2
TILES_MB = 8
TILES = 16
BLOCKS = 8
GROUP = 8
KF = 512
MOST = 8


def draw_queries(key, part):
    sample = jax.random.normal(jax.random.fold_in(key, 11), (MB, TILES_MB, TILE, QHEADS, HEAD), jnp.float32)
    return jnp.clip(sample, -8.0, 8.0).reshape(MB, TILES_MB, TILE, QHEADS * HEAD).astype(jnp.bfloat16)


def draw_keys(key, part):
    sample = jax.random.normal(jax.random.fold_in(key, 21), (BLOCKS, BLOCK, KV_HEADS, HEAD), jnp.float32)
    return jnp.clip(sample, -8.0, 8.0).reshape(BLOCKS, BLOCK, KV_HEADS * HEAD).astype(jnp.bfloat16)


def plant(entries, key, smallest, largest):
    extent = entries.shape
    index_at = [jax.random.randint(jax.random.fold_in(key, axis), (), 0, extent[axis]) for axis in range(len(extent))]
    entries = entries.at[tuple(index_at)].set(smallest)
    longest = extent.index(max(extent))
    index_at[longest] = (index_at[longest] + 1) % extent[longest]
    return entries.at[tuple(index_at)].set(largest)


def block_levels(rng, shape, cuts, low, top_value):
    def one(dim, blocks):
        draws = jax.random.uniform(jax.random.fold_in(jax.random.fold_in(rng, 6), dim), (blocks,), jnp.float32, low / len(cuts), top_value / len(cuts))
        return jnp.repeat(jnp.exp(draws), shape[dim] // blocks).reshape((-1,) + (1,) * (len(shape) - dim - 1))

    loudness = one(*cuts[0])
    for cut in cuts[1:]:
        loudness = loudness * one(*cut)
    return loudness


def routed_block(key, own, number, rows, number_of, top, most, slope):
    order = jax.random.permutation(key, number_of)
    packed, ordinary = load_shares(number_of, rows * top, most, slope, True), load_shares(number_of, rows * top, most, slope, False)
    places = jnp.arange(number_of)

    def named(tallies, rotation):
        used = int((tallies > 0).sum())
        fixed = max(1, used // 4)
        shifted = fixed + (places - fixed + rotation * (used - fixed)) % max(1, number_of - fixed)
        return jnp.zeros((number_of,), jnp.int32).at[order[jnp.where(places < fixed, places, shifted)]].set(jnp.asarray(tallies, jnp.int32))

    tallies = jnp.where(number % 4 == 0, named(packed, number // 4), named(ordinary, number - number // 4 - 1))
    mixed = jax.random.permutation(jax.random.fold_in(own, 3), number_of)
    source_of, taker = mixed[0:number_of // 2 * 2:2], mixed[1:number_of // 2 * 2:2]
    slack = jnp.minimum(tallies[source_of] - 1, most - tallies[taker]) // 2
    slack = jnp.where((source_of == order[0]) | (taker == order[0]) | (tallies[taker] == 0), 0, jnp.maximum(slack, 0))
    shifted = jax.random.randint(jax.random.fold_in(own, 4), (number_of // 2,), 0, 1 << 20) % (slack + 1)
    tallies = tallies.at[source_of].add(-shifted).at[taker].add(shifted)
    items = jnp.searchsorted(jnp.cumsum(tallies), jnp.arange(rows * top), side="right").astype(jnp.int32)
    grid = items.reshape(top, rows).T
    grid = grid[jax.random.permutation(jax.random.fold_in(own, 1), rows)]
    rotation = jax.random.randint(jax.random.fold_in(own, 2), (rows, 1), 0, top)
    return jnp.take_along_axis(grid, (jnp.arange(top)[None, :] + rotation) % top, axis=1)


def load_shares(count, total, bound, skew, full):
    weights = [(1 << 20) // math.isqrt(standing ** skew) + 1 for standing in range(1, count + 1)]
    largest = bound if full else min(bound, max(-(-total // count), total * weights[0] // sum(weights)))
    least = 1 if total - largest >= count - 1 else 0
    given, rest = [largest] + [least] * (count - 1), total - largest - least * (count - 1)
    while rest > 0:
        movable = [i for i in range(1, count) if given[i] < largest] or [i for i in range(1, count) if given[i] < bound]
        pool, budget = sum([weights[i] for i in movable]), rest
        for i in movable:
            extra = min(bound - given[i], max(1, budget * weights[i] // pool), rest)
            given[i] = given[i] + extra
            rest = rest - extra
    return np.array(given)


def gaussian(key, shape, scale, most, cuts=(), held_as=jnp.bfloat16):
    values = scale * jax.random.normal(key, shape, jnp.float32)
    if cuts:
        values = values * block_levels(key, shape, cuts, -0.22, 0.18)
    return jnp.clip(values, -most, most).astype(held_as)


def setup_inputs(seed: int = 0, part: int = 0) -> dict:
    seeds = jax.random.split(jax.random.key(seed), 7)
    own_keys = jax.random.split(jax.random.fold_in(seeds[6], part), 7)
    queries = draw_queries(jax.random.fold_in(jax.random.fold_in(seeds[6], part), 71), part)
    keys = draw_keys(jax.random.fold_in(jax.random.fold_in(seeds[6], part), 71), part)
    values = gaussian(own_keys[2], (BLOCKS, BLOCK, KF), 1.0, 6.0, ((0, 8), (2, 2)))
    tile_blocks_keys = jax.random.split(jax.random.fold_in(own_keys[3], 1), TILES // TILES_MB)
    tile_blocks_turns = jax.random.permutation(jax.random.fold_in(own_keys[3], 3), TILES // TILES_MB)
    tile_blocks = jax.vmap(lambda own, number: routed_block(jax.random.fold_in(own_keys[3], 2), own, number, TILES_MB, BLOCKS, TOP, MOST, 2))(tile_blocks_keys, tile_blocks_turns).reshape((TILES, TOP))
    block_place = jax.random.permutation(own_keys[4], BLOCKS).astype(jnp.int32)
    tile_offset = plant(jax.random.randint(own_keys[5], (TILES,), 0, BLOCK // TILE), jax.random.fold_in(own_keys[5], 1), 0, (BLOCK // TILE) - 1).astype(jnp.int32)
    return {"queries": queries, "keys": keys, "values": values, "tile_blocks": tile_blocks, "block_place": block_place, "tile_offset": tile_offset}


def partial_block(tile_query, key_block, value_block, horizon):
    scores = jnp.einsum('rcgh,kch->cgrk', tile_query.astype(jnp.float32), key_block.astype(jnp.float32)) * HEAD ** -0.5
    visible = jnp.arange(BLOCK, dtype=jnp.int32)[None, :] <= horizon[:, None]
    scores = jnp.where(visible[None, None], scores, -1e30)
    highest = jnp.max(scores, axis=3, keepdims=True)
    weights = jnp.exp(scores - highest)
    summed = jnp.sum(weights, axis=3, keepdims=True)
    rounded = lax.optimization_barrier(weights.astype(jnp.bfloat16)).astype(jnp.float32)
    blended = jnp.einsum('cgrk,kch->cgrh', rounded, value_block.astype(jnp.float32)) / summed
    return blended, (highest + jnp.log(summed))[..., 0]


def reference(queries, keys, values, tile_blocks, block_place, tile_offset):
    tile_count = queries.shape[0] * queries.shape[1]
    shaped = queries.reshape(tile_count, TILE, KV_HEADS, GROUP, HEAD)
    key_blocks = keys.reshape(keys.shape[0], BLOCK, KV_HEADS, HEAD)
    value_blocks = values.reshape(values.shape[0], BLOCK, KV_HEADS, HEAD)

    def one_tile(bundle):
        tile_query, block_list, offset = bundle
        own_block = jnp.max(block_list)
        horizon_own = (offset * TILE + jnp.arange(TILE, dtype=jnp.int32)).astype(jnp.int32)
        pieces = []
        masses = []
        for entry_index in range(TOP):
            owner_row = block_place[block_list[entry_index]]
            horizon = jnp.where(block_list[entry_index] == own_block, horizon_own, BLOCK).astype(jnp.int32)
            blended, mass = partial_block(tile_query, key_blocks[owner_row], value_blocks[owner_row], horizon)
            pieces.append(blended)
            masses.append(mass)
        stacked = jnp.stack(pieces)
        mass_all = jnp.stack(masses)
        highest = jnp.max(mass_all, axis=0, keepdims=True)
        share_all = jnp.exp(mass_all - highest)
        share_all = share_all / jnp.sum(share_all, axis=0, keepdims=True)
        result = jnp.sum(share_all[..., None] * stacked, axis=0)
        return result.transpose(2, 0, 1, 3).reshape(TILE, KV_HEADS * GROUP * HEAD).astype(jnp.bfloat16)

    output = lax.map(one_tile, (shaped, tile_blocks, tile_offset))
    return output.reshape(queries.shape)
```

```python
import functools

import jax
import jax.numpy as jnp
from jax import lax
from jax.experimental import pallas as pl
from jax.experimental.pallas import tpu as pltpu
from jax.sharding import PartitionSpec as P

HEAD = 128
SCALE = HEAD ** (-0.5) * 1.4426950408889634
KEYS = 256
STEP = 512
SMALL = 2.0**-60
LARGE = 2.0**100
PAD = 16


def prepare(me, tile_blocks, block_place, tile_offset, values, turned, slots, *, tile_rows):
    keys, features = values.shape
    for head in range(features // HEAD):
        for start in range(0, keys, 512):
            turned[head, :HEAD, start : start + 512] = values[
                start : start + 512, head * HEAD : (head + 1) * HEAD
            ].T
        turned[head, HEAD:, :] = jnp.where(
            lax.broadcasted_iota(jnp.int32, (PAD, keys), 0) == 0, 1.0, 0.0
        ).astype(turned.dtype)
    block_count = block_place.shape[0]
    tiles, top = tile_blocks.shape

    def find(block, mine):
        return jnp.where(block_place[block] == me[0], block, mine)

    mine = lax.fori_loop(0, block_count, find, 0)

    def visit(tile, count):
        entries = [tile_blocks[tile, entry] for entry in range(top)]
        own = functools.reduce(jnp.maximum, entries)
        named = functools.reduce(jnp.logical_or, [entry == mine for entry in entries])

        @pl.when(named)
        def _():
            slots[1 + count] = tile
            slots[1 + tiles + 1 + count] = jnp.where(
                own == mine, tile_offset[tile] * tile_rows, keys
            )

        return count + named.astype(jnp.int32)

    count = lax.fori_loop(0, tiles, visit, 0)
    slots[0] = count

    @pl.when(count % 2 == 1)
    def _():
        slots[1 + count] = slots[count]
        slots[1 + tiles + 1 + count] = slots[1 + tiles + count]


def attend(slots, queries, keys_ref, turned, partial, rotated, total, checks, *, tiles):
    devices, batches, tile_rows, width = queries.shape
    group = width // HEAD
    rows = tile_rows * group
    key_count = keys_ref.shape[0]
    pairs = (slots[0] + 1) // 2
    checks[...] = jnp.ones(checks.shape, jnp.float32)

    def tile_of(pair, side):
        tile = slots[1 + 2 * pair + side]
        return tile % devices, tile // devices

    def horizon_of(pair, side):
        return slots[2 + tiles + 2 * pair + side]

    def columns(pair):
        row = lax.broadcasted_iota(jnp.int32, (1, rows), 1) % tile_rows
        return jnp.concatenate([horizon_of(pair, side) + row for side in range(2)], axis=1)

    def scores(start, count):
        return (
            jnp.dot(
                keys_ref[pl.ds(start, count), :],
                rotated[...],
                preferred_element_type=jnp.float32,
            )
            * SCALE
        )

    def visible(start, count, limits):
        return (
            lax.broadcasted_iota(jnp.int32, (count, 2 * rows), 0) + start
            <= limits
        )

    def load(pair):
        for side in range(2):
            device, batch = tile_of(pair, side)
            tile = queries[device, batch]
            stacked = jnp.concatenate(
                [tile[:, part * HEAD : (part + 1) * HEAD] for part in range(group)], axis=0
            )
            rotated[:, side * rows : (side + 1) * rows] = stacked.T

    def run(start, count, limits):
        steps = count // KEYS
        offsets = [start + step * KEYS for step in range(steps)]
        ahead = [scores(offset, KEYS) for offset in offsets[:2]]
        added = None
        for step in range(steps):
            weights = jnp.exp2(ahead[step])
            if limits is not None:
                weights = jnp.where(visible(offsets[step], KEYS, limits), weights, 0.0)
            if step + 2 < steps:
                ahead.append(scores(offsets[step + 2], KEYS))
            new = jnp.dot(
                turned[:, pl.ds(offsets[step], KEYS)],
                weights.astype(jnp.bfloat16),
                preferred_element_type=jnp.float32,
            )
            added = new if added is None else added + new
        return added

    def finish(pair, summed, highest):
        mass = jnp.log2(summed) + highest
        high = mass.astype(jnp.bfloat16)
        middle = (mass - high.astype(jnp.float32)).astype(jnp.bfloat16)
        low = (mass - high.astype(jnp.float32) - middle.astype(jnp.float32)).astype(jnp.bfloat16)
        pad = lax.broadcasted_iota(jnp.int32, (PAD, 2 * rows), 0)
        terms = jnp.where(
            pad == 0,
            high.astype(jnp.float32),
            jnp.where(
                pad == 1,
                middle.astype(jnp.float32),
                jnp.where(pad == 2, low.astype(jnp.float32), 0.0),
            ),
        ).astype(jnp.bfloat16)
        blended = (total[:HEAD] * (1.0 / summed)).T.astype(jnp.bfloat16)
        for side in range(2):
            device, batch = tile_of(pair, side)
            part = slice(side * rows, (side + 1) * rows)
            partial[device, batch, :rows] = blended[part]
            partial[device, batch, rows:] = terms[:, part]

    def quick(pair, carry):
        load(pair)
        first = horizon_of(pair, 0)
        second = horizon_of(pair, 1)
        fewest = jnp.minimum(first, second)
        most = jnp.maximum(first, second)

        @pl.when(fewest == key_count)
        def _():
            total[...] = run(0, key_count, None)

        @pl.when(fewest < key_count)
        def _():
            limits = columns(pair)
            total[...] = jnp.zeros(total.shape, jnp.float32)
            full = (fewest + 1) // STEP
            last = jnp.minimum((most + tile_rows + STEP - 1) // STEP, key_count // STEP)

            def plain(step, carry):
                total[...] += run(pl.multiple_of(step * STEP, STEP), STEP, None)
                return carry

            def masked(step, carry):
                total[...] += run(pl.multiple_of(step * STEP, STEP), STEP, limits)
                return carry

            lax.fori_loop(0, full, plain, 0)
            lax.fori_loop(full, last, masked, 0)

        summed = total[HEAD : HEAD + 1, :]
        good = (summed > SMALL) & (summed < LARGE)
        checks[...] = jnp.minimum(checks[...], jnp.where(good, 1.0, 0.0))
        finish(pair, summed, 0.0)
        return carry

    lax.fori_loop(0, pairs, quick, 0)

    def exact(pair, carry):
        load(pair)
        limits = columns(pair)

        def measured(step):
            start = pl.multiple_of(step * KEYS, KEYS)
            return jnp.where(visible(start, KEYS, limits), scores(start, KEYS), -1e30)

        def highest_of(step, highest):
            return jnp.maximum(highest, jnp.max(measured(step), axis=0, keepdims=True))

        highest = lax.fori_loop(
            0, key_count // KEYS, highest_of, jnp.full((1, 2 * rows), -1e30, jnp.float32)
        )
        total[...] = jnp.zeros(total.shape, jnp.float32)

        def add(step, carry):
            weights = jnp.exp2(measured(step) - highest).astype(jnp.bfloat16)
            total[...] += jnp.dot(
                turned[:, pl.ds(pl.multiple_of(step * KEYS, KEYS), KEYS)],
                weights,
                preferred_element_type=jnp.float32,
            )
            return carry

        lax.fori_loop(0, key_count // KEYS, add, 0)
        finish(pair, total[HEAD : HEAD + 1, :], highest)
        return carry

    @pl.when(jnp.min(checks[...]) < 0.5)
    def _():
        lax.fori_loop(0, pairs, exact, 0)


def combine(me, tile_blocks, block_place, first, second, attended):
    devices, batches, padded, _ = first.shape
    top = tile_blocks.shape[1]
    rows = padded - PAD
    tile_rows = attended.shape[1]
    for batch in range(batches):
        owners = [
            block_place[tile_blocks[batch * devices + me[0], entry]] for entry in range(top)
        ]
        for half, returned in enumerate((first, second)):
            masses = []
            for owner in owners:
                terms = returned[owner, batch, rows:].astype(jnp.float32)
                masses.append(terms[0:1] + terms[1:2] + terms[2:3])
            highest = functools.reduce(jnp.maximum, masses)
            shares = [jnp.exp2(mass - highest) for mass in masses]
            inverse = 1.0 / functools.reduce(jnp.add, shares)
            stacked = jnp.concatenate([share * inverse for share in shares], axis=0)
            stacked = jnp.concatenate(
                [stacked, jnp.zeros((8 - top, rows), jnp.float32)], axis=0
            ).T
            blended = functools.reduce(
                jnp.add,
                [
                    stacked[:, entry : entry + 1] * returned[owner, batch, :rows].astype(jnp.float32)
                    for entry, owner in enumerate(owners)
                ],
            ).astype(jnp.bfloat16)
            for part in range(rows // tile_rows):
                column = (half * (rows // tile_rows) + part) * HEAD
                attended[batch, :, column : column + HEAD] = blended[
                    part * tile_rows : (part + 1) * tile_rows
                ]


def local(queries, keys, values, tile_blocks, block_place, tile_offset):
    devices = lax.axis_size("seq")
    batches, _, tile_rows, features = queries.shape
    _, key_count, key_features = keys.shape
    shared = key_features // HEAD
    width = features // shared
    rows = tile_rows * (width // HEAD)
    tiles = tile_blocks.shape[0]
    me = lax.axis_index("seq").astype(jnp.int32)[None]
    smem = pl.BlockSpec(memory_space=pltpu.SMEM)
    vmem = pl.BlockSpec(memory_space=pltpu.VMEM)
    turned, slots = pl.pallas_call(
        functools.partial(prepare, tile_rows=tile_rows),
        out_shape=(
            jax.ShapeDtypeStruct((shared, HEAD + PAD, key_count), jnp.bfloat16),
            jax.ShapeDtypeStruct((2 * tiles + 4,), jnp.int32),
        ),
        in_specs=[smem, smem, smem, smem, vmem],
        out_specs=(vmem, smem),
        name="prepare",
    )(me, tile_blocks, block_place, tile_offset, values[0])
    arrived = []
    for head in range(shared):
        tile = queries[:, 0, :, head * width : (head + 1) * width]
        outgoing = jnp.broadcast_to(tile[None], (devices,) + tile.shape)
        arrived.append(
            lax.all_to_all(outgoing, "seq", split_axis=0, concat_axis=0, tiled=True)
        )
    returned = []
    for head in range(shared):
        partial = pl.pallas_call(
            functools.partial(attend, tiles=tiles),
            grid=(1,),
            out_shape=jax.ShapeDtypeStruct(
                (devices, batches, rows + PAD, HEAD), jnp.bfloat16
            ),
            in_specs=[
                smem,
                vmem,
                pl.BlockSpec((None, key_count, HEAD), lambda i, head=head: (0, 0, head)),
                pl.BlockSpec((None, HEAD + PAD, key_count), lambda i, head=head: (head, 0, 0)),
            ],
            out_specs=vmem,
            scratch_shapes=[
                pltpu.VMEM((HEAD, 2 * rows), jnp.bfloat16),
                pltpu.VMEM((HEAD + PAD, 2 * rows), jnp.float32),
                pltpu.VMEM((1, 2 * rows), jnp.float32),
            ],
            name="attend",
        )(slots, arrived[head], keys, turned)
        returned.append(
            lax.all_to_all(partial, "seq", split_axis=0, concat_axis=0, tiled=True)
        )
    out = pl.pallas_call(
        combine,
        out_shape=jax.ShapeDtypeStruct((batches, tile_rows, features), jnp.bfloat16),
        in_specs=[smem, smem, smem, vmem, vmem],
        out_specs=vmem,
        name="combine",
    )(me, tile_blocks, block_place, *returned)
    return out[:, None]


def solution(mesh):
    placed = (
        P(None, ("groups", "seq"), None, "heads"),
        P(("groups", "seq"), None, "heads"),
        P(("groups", "seq"), None, "heads"),
        P("groups", None),
        P("groups"),
        P("groups"),
    )
    return jax.shard_map(
        local,
        mesh=mesh,
        in_specs=placed,
        out_specs=P(None, ("groups", "seq"), None, "heads"),
        check_vma=False,
    )
```

```python
import functools

import jax
import jax.numpy as jnp
from jax import lax
from jax.experimental import pallas as pl
from jax.experimental.pallas import tpu as pltpu
from jax.sharding import PartitionSpec as P

HEAD = 128
SCALE = HEAD ** (-0.5) * 1.4426950408889634
KEYS = 256
SMALL = 2.0**-60
LARGE = 2.0**100
PAD = 16


def prepare(me, tile_blocks, block_place, tile_offset, values, turned, slots, *, tile_rows):
    keys, features = values.shape
    for head in range(features // HEAD):
        for start in range(0, keys, 512):
            turned[head, :HEAD, start : start + 512] = values[
                start : start + 512, head * HEAD : (head + 1) * HEAD
            ].T
        turned[head, HEAD:, :] = jnp.where(
            lax.broadcasted_iota(jnp.int32, (PAD, keys), 0) == 0, 1.0, 0.0
        ).astype(turned.dtype)
    block_count = block_place.shape[0]
    tiles, top = tile_blocks.shape

    def find(block, mine):
        return jnp.where(block_place[block] == me[0], block, mine)

    mine = lax.fori_loop(0, block_count, find, 0)

    def visit(tile, counts, late):
        count = counts
        entries = [tile_blocks[tile, entry] for entry in range(top)]
        own = functools.reduce(jnp.maximum, entries) == mine
        named = functools.reduce(jnp.logical_or, [entry == mine for entry in entries])
        chosen = named & (own if late else jnp.logical_not(own))

        @pl.when(chosen)
        def _():
            slots[2 + count] = tile
            slots[3 + tiles + count] = tile_offset[tile] * tile_rows if late else keys

        return count + chosen.astype(jnp.int32)

    whole = lax.fori_loop(0, tiles, functools.partial(visit, late=False), 0)
    count = lax.fori_loop(0, tiles, functools.partial(visit, late=True), whole)
    slots[0] = whole // 2
    slots[1] = (count + 1) // 2

    @pl.when(count % 2 == 1)
    def _():
        slots[2 + count] = slots[1 + count]
        slots[3 + tiles + count] = slots[2 + tiles + count]


def attend(slots, queries, keys_ref, turned, partial, rotated, total, checks, *, tiles):
    devices, batches, tile_rows, width = queries.shape
    group = width // HEAD
    rows = tile_rows * group
    key_count = keys_ref.shape[0]
    columns = 2 * rows
    steps = key_count // (2 * KEYS)
    checks[...] = jnp.ones(checks.shape, jnp.float32)
    rotated[...] = jnp.zeros(rotated.shape, rotated.dtype)

    def tile_of(pair, side):
        tile = slots[2 + 2 * pair + side]
        return tile % devices, tile // devices

    def limits_of(pair):
        row = lax.broadcasted_iota(jnp.int32, (1, rows), 1) % tile_rows
        return jnp.concatenate(
            [slots[3 + tiles + 2 * pair + side] + row for side in range(2)], axis=1
        )

    def visible(start, limits):
        return lax.broadcasted_iota(jnp.int32, (KEYS, columns), 0) <= limits - start

    def load(pair, place):
        for side in range(2):
            device, batch = tile_of(pair, side)
            tile = queries[device, batch]
            stacked = jnp.concatenate(
                [tile[:, part * HEAD : (part + 1) * HEAD] for part in range(group)], axis=0
            )
            rotated[place, :HEAD, side * rows : (side + 1) * rows] = stacked.T

    def finish(pair, summed, highest):
        mass = jnp.log2(summed) + highest
        high = mass.astype(jnp.bfloat16)
        middle = (mass - high.astype(jnp.float32)).astype(jnp.bfloat16)
        low = (mass - high.astype(jnp.float32) - middle.astype(jnp.float32)).astype(jnp.bfloat16)
        pad = lax.broadcasted_iota(jnp.int32, (PAD, columns), 0)
        terms = jnp.where(
            pad == 0,
            high.astype(jnp.float32),
            jnp.where(
                pad == 1,
                middle.astype(jnp.float32),
                jnp.where(pad == 2, low.astype(jnp.float32), 0.0),
            ),
        ).astype(jnp.bfloat16)
        blended = (total[:HEAD] * (1.0 / summed)).T.astype(jnp.bfloat16)
        for side in range(2):
            device, batch = tile_of(pair, side)
            part = slice(side * rows, (side + 1) * rows)
            partial[device, batch, :rows] = blended[part]
            partial[device, batch, rows:] = terms[:, part]

    def quick(first, last, masked, accumulators):
        score = accumulators[:2], accumulators[2:4]
        value = accumulators[4:]

        def score_step(unit, place, step):
            start = (2 * step + unit) * KEYS
            block = keys_ref[start : start + KEYS]
            pltpu.matmul_push_rhs(rotated[place], 0, unit)
            pltpu.matmul_acc_lhs(
                score[unit][step % 2], jnp.concatenate([block, block], axis=1), 0
            )

        def value_step(unit, step, limits):
            start = (2 * step + unit) * KEYS
            weights = jnp.exp2(pltpu.matmul_pop(score[unit][step % 2]) * SCALE)
            if masked:
                weights = jnp.where(visible(start, limits), weights, 0.0)
            pltpu.matmul_push_rhs(weights.astype(jnp.bfloat16), 1, unit)
            pltpu.matmul_acc_lhs(value[unit], turned[:, start : start + KEYS], 1)

        def close(pair, real):
            total[...] = pltpu.matmul_pop(value[0]) + pltpu.matmul_pop(value[1])
            summed = total[HEAD : HEAD + 1, :]
            good = (summed > SMALL) & (summed < LARGE)
            checks[...] = jnp.minimum(checks[...], jnp.where(good | jnp.logical_not(real), 1.0, 0.0))
            finish(pair, summed, 0.0)

        for unit in range(2):
            for accumulator in score[unit] + value[unit : unit + 1]:
                pltpu.matmul_pop(accumulator)
        load(first, first % 2)
        for unit in range(2):
            score_step(unit, first % 2, 0)

        def body(pair, carry):
            place = pair % 2
            limits = limits_of(pair) if masked else None
            close(jnp.maximum(pair - 1, first), pair > first)
            load(jnp.minimum(pair + 1, last - 1), 1 - place)
            for step in range(steps):
                for unit in range(2):
                    if step + 1 < steps:
                        score_step(unit, place, step + 1)
                    else:
                        score_step(unit, 1 - place, 0)
                    value_step(unit, step, limits)
            return carry

        lax.fori_loop(first, last, body, 0)
        for unit in range(2):
            pltpu.matmul_pop(score[unit][0])
        close(last - 1, True)

    def exact(pair, carry, accumulators):
        score, value = accumulators[0], accumulators[4]
        load(pair, 0)
        limits = limits_of(pair)

        def measured(step):
            start = pl.multiple_of(step * KEYS, KEYS)
            block = keys_ref[pl.ds(start, KEYS), :]
            pltpu.matmul_push_rhs(rotated[0], 0, 0)
            pltpu.matmul_acc_lhs(score, jnp.concatenate([block, block], axis=1), 0)
            scores = pltpu.matmul_pop(score) * SCALE
            return jnp.where(visible(start, limits), scores, -1e30)

        def highest_of(step, highest):
            return jnp.maximum(highest, jnp.max(measured(step), axis=0, keepdims=True))

        highest = lax.fori_loop(
            0, key_count // KEYS, highest_of, jnp.full((1, columns), -1e30, jnp.float32)
        )

        def add(step, carry):
            weights = jnp.exp2(measured(step) - highest).astype(jnp.bfloat16)
            pltpu.matmul_push_rhs(weights, 1, 0)
            pltpu.matmul_acc_lhs(
                value, turned[:, pl.ds(pl.multiple_of(step * KEYS, KEYS), KEYS)], 1
            )
            return carry

        lax.fori_loop(0, key_count // KEYS, add, 0)
        total[...] = pltpu.matmul_pop(value)
        finish(pair, total[HEAD : HEAD + 1, :], highest)
        return carry

    def every(*accumulators):
        @pl.when(slots[0] > 0)
        def _():
            quick(0, slots[0], False, accumulators)

        @pl.when(slots[1] > slots[0])
        def _():
            quick(slots[0], slots[1], True, accumulators)

        @pl.when(jnp.min(checks[...]) < 0.5)
        def _():
            lax.fori_loop(
                0, slots[1], functools.partial(exact, accumulators=accumulators), 0
            )

    pl.run_scoped(
        every,
        *[pltpu.ACC(unit)((KEYS, columns), jnp.float32) for unit in (0, 0, 1, 1)],
        *[pltpu.ACC(unit)((HEAD + PAD, columns), jnp.float32) for unit in (0, 1)],
    )


def combine(me, tile_blocks, block_place, first, second, attended):
    devices, batches, padded, _ = first.shape
    top = tile_blocks.shape[1]
    rows = padded - PAD
    tile_rows = attended.shape[1]
    for batch in range(batches):
        owners = [
            block_place[tile_blocks[batch * devices + me[0], entry]] for entry in range(top)
        ]
        for half, returned in enumerate((first, second)):
            masses = []
            for owner in owners:
                terms = returned[owner, batch, rows:].astype(jnp.float32)
                masses.append(terms[0:1] + terms[1:2] + terms[2:3])
            highest = functools.reduce(jnp.maximum, masses)
            shares = [jnp.exp2(mass - highest) for mass in masses]
            inverse = 1.0 / functools.reduce(jnp.add, shares)
            stacked = jnp.concatenate([share * inverse for share in shares], axis=0)
            stacked = jnp.concatenate(
                [stacked, jnp.zeros((8 - top, rows), jnp.float32)], axis=0
            ).T
            blended = functools.reduce(
                jnp.add,
                [
                    stacked[:, entry : entry + 1] * returned[owner, batch, :rows].astype(jnp.float32)
                    for entry, owner in enumerate(owners)
                ],
            ).astype(jnp.bfloat16)
            for part in range(rows // tile_rows):
                column = (half * (rows // tile_rows) + part) * HEAD
                attended[batch, :, column : column + HEAD] = blended[
                    part * tile_rows : (part + 1) * tile_rows
                ]


def local(queries, keys, values, tile_blocks, block_place, tile_offset):
    devices = lax.axis_size("seq")
    batches, _, tile_rows, features = queries.shape
    _, key_count, key_features = keys.shape
    shared = key_features // HEAD
    width = features // shared
    rows = tile_rows * (width // HEAD)
    tiles = tile_blocks.shape[0]
    me = lax.axis_index("seq").astype(jnp.int32)[None]
    smem = pl.BlockSpec(memory_space=pltpu.SMEM)
    vmem = pl.BlockSpec(memory_space=pltpu.VMEM)
    turned, slots = pl.pallas_call(
        functools.partial(prepare, tile_rows=tile_rows),
        out_shape=(
            jax.ShapeDtypeStruct((shared, HEAD + PAD, key_count), jnp.bfloat16),
            jax.ShapeDtypeStruct((2 * tiles + 5,), jnp.int32),
        ),
        in_specs=[smem, smem, smem, smem, vmem],
        out_specs=(vmem, smem),
        cost_estimate=pl.CostEstimate(flops=10**10, transcendentals=0, bytes_accessed=2**22),
        name="prepare",
    )(me, tile_blocks, block_place, tile_offset, values[0])
    arrived = []
    for head in range(shared):
        tile = queries[:, 0, :, head * width : (head + 1) * width]
        outgoing = jnp.broadcast_to(tile[None], (devices,) + tile.shape)
        arrived.append(
            lax.all_to_all(outgoing, "seq", split_axis=0, concat_axis=0, tiled=True)
        )
    returned = []
    for head in range(shared):
        partial = pl.pallas_call(
            functools.partial(attend, tiles=tiles),
            grid=(1,),
            out_shape=jax.ShapeDtypeStruct(
                (devices, batches, rows + PAD, HEAD), jnp.bfloat16
            ),
            in_specs=[
                smem,
                vmem,
                pl.BlockSpec((None, key_count, HEAD), lambda i, head=head: (0, 0, head)),
                pl.BlockSpec((None, HEAD + PAD, key_count), lambda i, head=head: (head, 0, 0)),
            ],
            out_specs=vmem,
            scratch_shapes=[
                pltpu.VMEM((2, 2 * HEAD, 2 * rows), jnp.bfloat16),
                pltpu.VMEM((HEAD + PAD, 2 * rows), jnp.float32),
                pltpu.VMEM((1, 2 * rows), jnp.float32),
            ],
            cost_estimate=pl.CostEstimate(flops=10**10, transcendentals=0, bytes_accessed=2**22),
            name="attend",
        )(slots, arrived[head], keys, turned)
        returned.append(
            lax.all_to_all(partial, "seq", split_axis=0, concat_axis=0, tiled=True)
        )
    out = pl.pallas_call(
        combine,
        out_shape=jax.ShapeDtypeStruct((batches, tile_rows, features), jnp.bfloat16),
        in_specs=[smem, smem, smem, vmem, vmem],
        out_specs=vmem,
        name="combine",
    )(me, tile_blocks, block_place, *returned)
    return out[:, None]


def solution(mesh):
    placed = (
        P(None, ("groups", "seq"), None, "heads"),
        P(("groups", "seq"), None, "heads"),
        P(("groups", "seq"), None, "heads"),
        P("groups", None),
        P("groups"),
        P("groups"),
    )
    return jax.shard_map(
        local,
        mesh=mesh,
        in_specs=placed,
        out_specs=P(None, ("groups", "seq"), None, "heads"),
        check_vma=False,
    )
```

```python
import functools

import jax
import jax.numpy as jnp
from jax import lax
from jax.experimental import pallas as pl
from jax.experimental.pallas import tpu as pltpu
from jax.sharding import PartitionSpec as P


HEAD = 128
SCALE = HEAD ** (-0.5) * 1.4426950408889634
KEYS = 256
SMALL = 2.0**-60
LARGE = 2.0**100
PAD = 16
TERMS = 4


def prepare(me, tile_blocks, block_place, tile_offset, values, turned, slots, *, tile_rows):
    keys, features = values.shape
    for head in range(features // HEAD):
        for start in range(0, keys, 512):
            turned[head, :HEAD, start : start + 512] = values[
                start : start + 512, head * HEAD : (head + 1) * HEAD
            ].T
        turned[head, HEAD:, :] = jnp.where(
            lax.broadcasted_iota(jnp.int32, (PAD, keys), 0) == 0, 1.0, 0.0
        ).astype(turned.dtype)
    block_count = block_place.shape[0]
    tiles, top = tile_blocks.shape

    def find(block, mine):
        return jnp.where(block_place[block] == me[0], block, mine)

    mine = lax.fori_loop(0, block_count, find, 0)

    def visit(tile, counts, late):
        count = counts
        entries = [tile_blocks[tile, entry] for entry in range(top)]
        own = functools.reduce(jnp.maximum, entries) == mine
        named = functools.reduce(jnp.logical_or, [entry == mine for entry in entries])
        chosen = named & (own if late else jnp.logical_not(own))

        @pl.when(chosen)
        def _():
            slots[2 + count] = tile
            slots[3 + tiles + count] = tile_offset[tile] * tile_rows if late else keys

        return count + chosen.astype(jnp.int32)

    whole = lax.fori_loop(0, tiles, functools.partial(visit, late=False), 0)
    count = lax.fori_loop(0, tiles, functools.partial(visit, late=True), whole)
    slots[0] = whole // 2
    slots[1] = (count + 1) // 2

    @pl.when(count % 2 == 1)
    def _():
        slots[2 + count] = slots[1 + count]
        slots[3 + tiles + count] = slots[2 + tiles + count]


def attend(slots, queries, keys_ref, turned, partial, rotated, total, checks, *, tiles):
    devices, batches, tile_rows, width = queries.shape
    group = width // HEAD
    rows = tile_rows * group
    key_count = keys_ref.shape[0]
    columns = 2 * rows
    steps = key_count // (2 * KEYS)
    checks[...] = jnp.ones(checks.shape, jnp.float32)
    rotated[...] = jnp.zeros(rotated.shape, rotated.dtype)

    def tile_of(pair, side):
        tile = slots[2 + 2 * pair + side]
        return tile % devices, tile // devices

    def limits_of(pair):
        row = lax.broadcasted_iota(jnp.int32, (1, rows), 1) % tile_rows
        return jnp.concatenate(
            [slots[3 + tiles + 2 * pair + side] + row for side in range(2)], axis=1
        )

    def visible(start, limits):
        return lax.broadcasted_iota(jnp.int32, (KEYS, columns), 0) <= limits - start

    def load(pair, place):
        for side in range(2):
            device, batch = tile_of(pair, side)
            tile = queries[device, batch]
            stacked = jnp.concatenate(
                [tile[:, part * HEAD : (part + 1) * HEAD] for part in range(group)], axis=0
            )
            rotated[place, :HEAD, side * rows : (side + 1) * rows] = stacked.T

    def finish(pair, summed, highest):
        mass = jnp.log2(summed) + highest
        high = mass.astype(jnp.bfloat16)
        middle = (mass - high.astype(jnp.float32)).astype(jnp.bfloat16)
        low = (mass - high.astype(jnp.float32) - middle.astype(jnp.float32)).astype(jnp.bfloat16)
        pad = lax.broadcasted_iota(jnp.int32, (TERMS * batches, columns), 0)
        terms = jnp.where(
            pad % TERMS == 0,
            high.astype(jnp.float32),
            jnp.where(
                pad % TERMS == 1,
                middle.astype(jnp.float32),
                jnp.where(pad % TERMS == 2, low.astype(jnp.float32), 0.0),
            ),
        )
        blended = (total[:HEAD] * (1.0 / summed)).T.astype(jnp.bfloat16)
        for side in range(2):
            device, batch = tile_of(pair, side)
            part = slice(side * rows, (side + 1) * rows)
            partial[device, pl.ds(pl.multiple_of(batch * rows, rows), rows)] = blended[part]
            held = partial[device, batches * rows :].astype(jnp.float32)
            partial[device, batches * rows :] = jnp.where(
                pad[:, part] // TERMS == batch, terms[:, part], held
            ).astype(jnp.bfloat16)

    def quick(first, last, masked, accumulators):
        score = accumulators[:2], accumulators[2:4]
        value = accumulators[4:]

        def score_step(unit, place, step):
            start = (2 * step + unit) * KEYS
            block = keys_ref[start : start + KEYS]
            pltpu.matmul_push_rhs(rotated[place], 0, unit)
            pltpu.matmul_acc_lhs(
                score[unit][step % 2], jnp.concatenate([block, block], axis=1), 0
            )

        def value_step(unit, step, limits):
            start = (2 * step + unit) * KEYS
            weights = jnp.exp2(pltpu.matmul_pop(score[unit][step % 2]) * SCALE)
            if masked:
                weights = jnp.where(visible(start, limits), weights, 0.0)
            pltpu.matmul_push_rhs(weights.astype(jnp.bfloat16), 1, unit)
            pltpu.matmul_acc_lhs(value[unit], turned[:, start : start + KEYS], 1)

        def close(pair, real):
            total[...] = pltpu.matmul_pop(value[0]) + pltpu.matmul_pop(value[1])
            summed = total[HEAD : HEAD + 1, :]
            good = (summed > SMALL) & (summed < LARGE)
            checks[...] = jnp.minimum(checks[...], jnp.where(good | jnp.logical_not(real), 1.0, 0.0))
            finish(pair, summed, 0.0)

        for unit in range(2):
            for accumulator in score[unit] + value[unit : unit + 1]:
                pltpu.matmul_pop(accumulator)
        load(first, first % 2)
        for unit in range(2):
            score_step(unit, first % 2, 0)

        def body(pair, carry):
            place = pair % 2
            limits = limits_of(pair) if masked else None
            close(jnp.maximum(pair - 1, first), pair > first)
            load(jnp.minimum(pair + 1, last - 1), 1 - place)
            for step in range(steps):
                for unit in range(2):
                    if step + 1 < steps:
                        score_step(unit, place, step + 1)
                    else:
                        score_step(unit, 1 - place, 0)
                    value_step(unit, step, limits)
            return carry

        lax.fori_loop(first, last, body, 0)
        for unit in range(2):
            pltpu.matmul_pop(score[unit][0])
        close(last - 1, True)

    def exact(pair, carry, accumulators):
        score, value = accumulators[0], accumulators[4]
        load(pair, 0)
        limits = limits_of(pair)

        def measured(step):
            start = pl.multiple_of(step * KEYS, KEYS)
            block = keys_ref[pl.ds(start, KEYS), :]
            pltpu.matmul_push_rhs(rotated[0], 0, 0)
            pltpu.matmul_acc_lhs(score, jnp.concatenate([block, block], axis=1), 0)
            scores = pltpu.matmul_pop(score) * SCALE
            return jnp.where(visible(start, limits), scores, -1e30)

        def highest_of(step, highest):
            return jnp.maximum(highest, jnp.max(measured(step), axis=0, keepdims=True))

        highest = lax.fori_loop(
            0, key_count // KEYS, highest_of, jnp.full((1, columns), -1e30, jnp.float32)
        )

        def add(step, carry):
            weights = jnp.exp2(measured(step) - highest).astype(jnp.bfloat16)
            pltpu.matmul_push_rhs(weights, 1, 0)
            pltpu.matmul_acc_lhs(
                value, turned[:, pl.ds(pl.multiple_of(step * KEYS, KEYS), KEYS)], 1
            )
            return carry

        lax.fori_loop(0, key_count // KEYS, add, 0)
        total[...] = pltpu.matmul_pop(value)
        finish(pair, total[HEAD : HEAD + 1, :], highest)
        return carry

    def every(*accumulators):
        @pl.when(slots[0] > 0)
        def _():
            quick(0, slots[0], False, accumulators)

        @pl.when(slots[1] > slots[0])
        def _():
            quick(slots[0], slots[1], True, accumulators)

        @pl.when(jnp.min(checks[...]) < 0.5)
        def _():
            lax.fori_loop(
                0, slots[1], functools.partial(exact, accumulators=accumulators), 0
            )

    pl.run_scoped(
        every,
        *[pltpu.ACC(unit)((KEYS, columns), jnp.float32) for unit in (0, 0, 1, 1)],
        *[pltpu.ACC(unit)((HEAD + PAD, columns), jnp.float32) for unit in (0, 1)],
    )


def combine(me, tile_blocks, block_place, returned, *rest, tile_rows):
    attended = rest[-1]
    devices, padded, _ = returned.shape
    batches = attended.shape[0]
    top = tile_blocks.shape[1]
    rows = padded // batches - TERMS
    start = 0
    for earlier in rest[:-1]:
        attended[:, :, : earlier.shape[2]] = earlier[...]
        start = earlier.shape[2]
    for batch in range(batches):
        owners = [
            block_place[tile_blocks[batch * devices + me[0], entry]] for entry in range(top)
        ]
        masses = []
        for owner in owners:
            terms = returned[owner, batches * rows :].astype(jnp.float32)
            first = batch * TERMS
            masses.append(
                terms[first : first + 1] + terms[first + 1 : first + 2] + terms[first + 2 : first + 3]
            )
        highest = functools.reduce(jnp.maximum, masses)
        shares = [jnp.exp2(mass - highest) for mass in masses]
        inverse = 1.0 / functools.reduce(jnp.add, shares)
        stacked = jnp.concatenate(
            [share * inverse for share in shares] + [jnp.zeros((8 - top, rows), jnp.float32)],
            axis=0,
        ).T
        blended = functools.reduce(
            jnp.add,
            [
                stacked[:, entry : entry + 1]
                * returned[owner, batch * rows : (batch + 1) * rows].astype(jnp.float32)
                for entry, owner in enumerate(owners)
            ],
        ).astype(jnp.bfloat16)
        for part in range(rows // tile_rows):
            column = start + part * HEAD
            attended[batch, :, column : column + HEAD] = blended[
                part * tile_rows : (part + 1) * tile_rows
            ]


def local(queries, keys, values, tile_blocks, block_place, tile_offset):
    devices = lax.axis_size("seq")
    batches, _, tile_rows, features = queries.shape
    _, key_count, key_features = keys.shape
    shared = key_features // HEAD
    width = features // shared
    rows = tile_rows * (width // HEAD)
    tiles = tile_blocks.shape[0]
    me = lax.axis_index("seq").astype(jnp.int32)[None]
    smem = pl.BlockSpec(memory_space=pltpu.SMEM)
    vmem = pl.BlockSpec(memory_space=pltpu.VMEM)
    turned, slots = pl.pallas_call(
        functools.partial(prepare, tile_rows=tile_rows),
        out_shape=(
            jax.ShapeDtypeStruct((shared, HEAD + PAD, key_count), jnp.bfloat16),
            jax.ShapeDtypeStruct((2 * tiles + 5,), jnp.int32),
        ),
        in_specs=[smem, smem, smem, smem, vmem],
        out_specs=(vmem, smem),
        cost_estimate=pl.CostEstimate(flops=10**10, transcendentals=0, bytes_accessed=2**22),
        name="prepare",
    )(me, tile_blocks, block_place, tile_offset, values[0])
    arrived = []
    for head in range(shared):
        tile = queries[:, 0, :, head * width : (head + 1) * width]
        outgoing = jnp.broadcast_to(tile[None], (devices,) + tile.shape)
        arrived.append(
            lax.all_to_all(outgoing, "seq", split_axis=0, concat_axis=0, tiled=True)
        )
    returned = []
    for head in range(shared):
        partial = pl.pallas_call(
            functools.partial(attend, tiles=tiles),
            grid=(1,),
            out_shape=jax.ShapeDtypeStruct(
                (devices, batches * (rows + TERMS), HEAD), jnp.bfloat16
            ),
            in_specs=[
                smem,
                vmem,
                pl.BlockSpec((None, key_count, HEAD), lambda i, head=head: (0, 0, head)),
                pl.BlockSpec((None, HEAD + PAD, key_count), lambda i, head=head: (head, 0, 0)),
            ],
            out_specs=vmem,
            scratch_shapes=[
                pltpu.VMEM((2, 2 * HEAD, 2 * rows), jnp.bfloat16),
                pltpu.VMEM((HEAD + PAD, 2 * rows), jnp.float32),
                pltpu.VMEM((1, 2 * rows), jnp.float32),
            ],
            cost_estimate=pl.CostEstimate(flops=10**10, transcendentals=0, bytes_accessed=2**22),
            name="attend",
        )(slots, arrived[head], keys, turned)
        returned.append(
            lax.all_to_all(partial, "seq", split_axis=0, concat_axis=0, tiled=True)
        )
    out = ()
    for head in range(shared):
        out = (
            pl.pallas_call(
                functools.partial(combine, tile_rows=tile_rows),
                out_shape=jax.ShapeDtypeStruct(
                    (batches, tile_rows, (head + 1) * width), jnp.bfloat16
                ),
                in_specs=[smem, smem, smem, vmem] + [vmem] * len(out),
                out_specs=vmem,
                cost_estimate=pl.CostEstimate(
                    flops=2 * 10**9, transcendentals=0, bytes_accessed=2**20
                ),
                name="combine",
            )(me, tile_blocks, block_place, returned[head], *out),
        )
    return out[0][:, None]


def solution(mesh):
    placed = (
        P(None, ("groups", "seq"), None, "heads"),
        P(("groups", "seq"), None, "heads"),
        P(("groups", "seq"), None, "heads"),
        P("groups", None),
        P("groups"),
        P("groups"),
    )

    return jax.shard_map(
        local,
        mesh=mesh,
        in_specs=placed,
        out_specs=P(None, ("groups", "seq"), None, "heads"),
        check_vma=False,
    )
```

```python
import functools

import jax
import jax.numpy as jnp
from jax import lax
from jax.experimental import pallas as pl
from jax.experimental.pallas import tpu as pltpu
from jax.sharding import PartitionSpec as P


HEAD = 128
SCALE = HEAD ** (-0.5) * 1.4426950408889634
KEYS = 256
GRANT = 36 * 2**20
SMALL = 2.0**-60
LARGE = 2.0**100
TERMS = 4


def prepare(me, tile_blocks, block_place, tile_offset, values, turned, slots, *, tile_rows):
    keys, features = values.shape
    for head in range(features // HEAD):
        for start in range(0, keys, 512):
            turned[head, :, start : start + 512] = values[
                start : start + 512, head * HEAD : (head + 1) * HEAD
            ].T
    block_count = block_place.shape[0]
    tiles, top = tile_blocks.shape

    def find(block, mine):
        return jnp.where(block_place[block] == me[0], block, mine)

    mine = lax.fori_loop(0, block_count, find, 0)

    def visit(tile, counts, late):
        count = counts
        entries = [tile_blocks[tile, entry] for entry in range(top)]
        own = functools.reduce(jnp.maximum, entries) == mine
        named = functools.reduce(jnp.logical_or, [entry == mine for entry in entries])
        chosen = named & (own if late else jnp.logical_not(own))

        @pl.when(chosen)
        def _():
            slots[2 + count] = tile
            slots[3 + tiles + count] = tile_offset[tile] * tile_rows if late else keys

        return count + chosen.astype(jnp.int32)

    whole = lax.fori_loop(0, tiles, functools.partial(visit, late=False), 0)
    count = lax.fori_loop(0, tiles, functools.partial(visit, late=True), whole)
    slots[0] = whole // 2
    slots[1] = (count + 1) // 2

    @pl.when(count % 2 == 1)
    def _():
        slots[2 + count] = slots[1 + count]
        slots[3 + tiles + count] = slots[2 + tiles + count]


def attend(slots, queries, all_keys, turned, partial, rotated, total, checks, *, tiles, head):
    devices, batches, tile_rows, width = queries.shape
    group = width // HEAD
    rows = tile_rows * group
    keys_ref = all_keys.at[:, head * HEAD : (head + 1) * HEAD]
    turned = turned.at[head]
    key_count = all_keys.shape[0]
    columns = 2 * rows
    steps = key_count // (2 * KEYS)
    checks[...] = jnp.ones(checks.shape, jnp.float32)
    rotated[...] = jnp.zeros(rotated.shape, rotated.dtype)

    def tile_of(pair, side):
        tile = slots[2 + 2 * pair + side]
        return tile % devices, tile // devices

    def limits_of(pair):
        row = lax.broadcasted_iota(jnp.int32, (1, rows), 1) % tile_rows
        return jnp.concatenate(
            [slots[3 + tiles + 2 * pair + side] + row for side in range(2)], axis=1
        )

    def visible(start, limits):
        return lax.broadcasted_iota(jnp.int32, (KEYS, columns), 0) <= limits - start

    def load(pair, place):
        for side in range(2):
            device, batch = tile_of(pair, side)
            tile = queries[device, batch]
            stacked = jnp.concatenate(
                [tile[:, part * HEAD : (part + 1) * HEAD] for part in range(group)], axis=0
            )
            rotated[place, :HEAD, side * rows : (side + 1) * rows] = stacked.T

    def finish(pair, summed, highest):
        mass = jnp.log2(summed) + highest
        high = mass.astype(jnp.bfloat16)
        middle = (mass - high.astype(jnp.float32)).astype(jnp.bfloat16)
        low = (mass - high.astype(jnp.float32) - middle.astype(jnp.float32)).astype(jnp.bfloat16)
        pad = lax.broadcasted_iota(jnp.int32, (TERMS * batches, columns), 0)
        terms = jnp.where(
            pad % TERMS == 0,
            high.astype(jnp.float32),
            jnp.where(
                pad % TERMS == 1,
                middle.astype(jnp.float32),
                jnp.where(pad % TERMS == 2, low.astype(jnp.float32), 0.0),
            ),
        )
        blended = (total[:HEAD] * (1.0 / summed)).T.astype(jnp.bfloat16)
        for side in range(2):
            device, batch = tile_of(pair, side)
            part = slice(side * rows, (side + 1) * rows)
            partial[device, pl.ds(pl.multiple_of(batch * rows, rows), rows)] = blended[part]
            held = partial[device, batches * rows :].astype(jnp.float32)
            partial[device, batches * rows :] = jnp.where(
                pad[:, part] // TERMS == batch, terms[:, part], held
            ).astype(jnp.bfloat16)

    def quick(first, last, masked, accumulators):
        score = accumulators[:2], accumulators[2:4]
        value = accumulators[4:]

        def score_step(unit, place, step):
            start = (2 * step + unit) * KEYS
            block = keys_ref[start : start + KEYS]
            pltpu.matmul_push_rhs(rotated[place], 0, unit)
            pltpu.matmul_acc_lhs(
                score[unit][step % 2], jnp.concatenate([block, block], axis=1), 0
            )

        def value_step(unit, step, limits):
            start = (2 * step + unit) * KEYS
            weights = jnp.exp2(pltpu.matmul_pop(score[unit][step % 2]) * SCALE)
            if masked:
                weights = jnp.where(visible(start, limits), weights, 0.0)
            pltpu.matmul_push_rhs(weights.astype(jnp.bfloat16), 1, unit)
            pltpu.matmul_acc_lhs(value[unit], turned[:, start : start + KEYS], 1)
            return jnp.sum(weights.reshape(KEYS // 8, 8, columns), axis=0)

        def close(pair, real):
            total[:HEAD] = pltpu.matmul_pop(value[0]) + pltpu.matmul_pop(value[1])
            summed = jnp.sum(total[HEAD:], axis=0, keepdims=True)
            good = (summed > SMALL) & (summed < LARGE)
            checks[...] = jnp.minimum(checks[...], jnp.where(good | jnp.logical_not(real), 1.0, 0.0))
            finish(pair, summed, 0.0)

        for unit in range(2):
            for accumulator in score[unit] + value[unit : unit + 1]:
                pltpu.matmul_pop(accumulator)
        total[HEAD:] = jnp.ones((8, columns), jnp.float32)
        load(first, first % 2)
        for unit in range(2):
            score_step(unit, first % 2, 0)

        def body(pair, carry):
            place = pair % 2
            limits = limits_of(pair) if masked else None
            close(jnp.maximum(pair - 1, first), pair > first)
            load(jnp.minimum(pair + 1, last - 1), 1 - place)
            for step in range(steps):
                for unit in range(2):
                    if step + 1 < steps:
                        score_step(unit, place, step + 1)
                    else:
                        score_step(unit, 1 - place, 0)
                    added = value_step(unit, step, limits)
                    whole = added if step + unit == 0 else whole + added
            total[HEAD:] = whole
            return carry

        lax.fori_loop(first, last, body, 0)
        for unit in range(2):
            pltpu.matmul_pop(score[unit][0])
        close(last - 1, True)

    def exact(pair, carry, accumulators):
        score, value = accumulators[0], accumulators[4]
        load(pair, 0)
        limits = limits_of(pair)

        def measured(step):
            start = pl.multiple_of(step * KEYS, KEYS)
            block = keys_ref[pl.ds(start, KEYS), :]
            pltpu.matmul_push_rhs(rotated[0], 0, 0)
            pltpu.matmul_acc_lhs(score, jnp.concatenate([block, block], axis=1), 0)
            scores = pltpu.matmul_pop(score) * SCALE
            return jnp.where(visible(start, limits), scores, -1e30)

        def highest_of(step, highest):
            return jnp.maximum(highest, jnp.max(measured(step), axis=0, keepdims=True))

        highest = lax.fori_loop(
            0, key_count // KEYS, highest_of, jnp.full((1, columns), -1e30, jnp.float32)
        )

        def add(step, summed):
            weights = jnp.exp2(measured(step) - highest)
            pltpu.matmul_push_rhs(weights.astype(jnp.bfloat16), 1, 0)
            pltpu.matmul_acc_lhs(
                value, turned[:, pl.ds(pl.multiple_of(step * KEYS, KEYS), KEYS)], 1
            )
            return summed + jnp.sum(weights, axis=0, keepdims=True)

        summed = lax.fori_loop(
            0, key_count // KEYS, add, jnp.zeros((1, columns), jnp.float32)
        )
        total[:HEAD] = pltpu.matmul_pop(value)
        finish(pair, summed, highest)
        return carry

    def every(*accumulators):
        @pl.when(slots[0] > 0)
        def _():
            quick(0, slots[0], False, accumulators)

        @pl.when(slots[1] > slots[0])
        def _():
            quick(slots[0], slots[1], True, accumulators)

        @pl.when(jnp.min(checks[...]) < 0.5)
        def _():
            lax.fori_loop(
                0, slots[1], functools.partial(exact, accumulators=accumulators), 0
            )

    pl.run_scoped(
        every,
        *[pltpu.ACC(unit)((KEYS, columns), jnp.float32) for unit in (0, 0, 1, 1)],
        *[pltpu.ACC(unit)((HEAD, columns), jnp.float32) for unit in (0, 1)],
    )


def combine(me, tile_blocks, block_place, returned, *rest, tile_rows):
    *rest, attended = rest
    devices, padded, _ = returned.shape
    batches = attended.shape[0]
    top = tile_blocks.shape[1]
    rows = padded // batches - TERMS
    start = 0
    for earlier in rest:
        attended[:, :, : earlier.shape[2]] = earlier[...]
        start = earlier.shape[2]
    for batch in range(batches):
        owners = [
            block_place[tile_blocks[batch * devices + me[0], entry]] for entry in range(top)
        ]
        masses = []
        for owner in owners:
            terms = returned[owner, batches * rows :].astype(jnp.float32)
            first = batch * TERMS
            masses.append(
                terms[first : first + 1] + terms[first + 1 : first + 2] + terms[first + 2 : first + 3]
            )
        highest = functools.reduce(jnp.maximum, masses)
        shares = [jnp.exp2(mass - highest) for mass in masses]
        inverse = 1.0 / functools.reduce(jnp.add, shares)
        stacked = jnp.concatenate(
            [share * inverse for share in shares] + [jnp.zeros((8 - top, rows), jnp.float32)],
            axis=0,
        ).T
        blended = functools.reduce(
            jnp.add,
            [
                stacked[:, entry : entry + 1]
                * returned[owner, batch * rows : (batch + 1) * rows].astype(jnp.float32)
                for entry, owner in enumerate(owners)
            ],
        ).astype(jnp.bfloat16)
        for part in range(rows // tile_rows):
            column = start + part * HEAD
            attended[batch, :, column : column + HEAD] = blended[
                part * tile_rows : (part + 1) * tile_rows
            ]


def near(array):
    return pltpu.with_memory_space_constraint(array, pltpu.VMEM)


def local(queries, keys, values, tile_blocks, block_place, tile_offset):
    devices = lax.axis_size("seq")
    batches, _, tile_rows, features = queries.shape
    _, key_count, key_features = keys.shape
    shared = key_features // HEAD
    width = features // shared
    rows = tile_rows * (width // HEAD)
    tiles = tile_blocks.shape[0]
    me = lax.axis_index("seq").astype(jnp.int32)[None]
    smem = pl.BlockSpec(memory_space=pltpu.SMEM)
    vmem = pl.BlockSpec(memory_space=pltpu.VMEM)
    turned, slots = pl.pallas_call(
        functools.partial(prepare, tile_rows=tile_rows),
        out_shape=(
            jax.ShapeDtypeStruct((shared, HEAD, key_count), jnp.bfloat16),
            jax.ShapeDtypeStruct((2 * tiles + 5,), jnp.int32),
        ),
        in_specs=[smem, smem, smem, smem, vmem],
        out_specs=(vmem, smem),
        cost_estimate=pl.CostEstimate(flops=10**10, transcendentals=0, bytes_accessed=2**22),
        compiler_params=pltpu.CompilerParams(vmem_limit_bytes=GRANT),
            name="prepare",
    )(me, tile_blocks, block_place, tile_offset, values[0])
    arrived = []
    for head in range(shared):
        source = lax.optimization_barrier(queries) if head else queries
        tile = source[:, 0, :, head * width : (head + 1) * width]
        outgoing = jnp.broadcast_to(tile[None], (devices,) + tile.shape)
        arrived.append(
            lax.all_to_all(outgoing, "seq", split_axis=0, concat_axis=0, tiled=True)
        )
    close_keys = near(keys[0])
    close_turned = near(turned)
    returned = []
    for head in range(shared):
        partial = pl.pallas_call(
            functools.partial(attend, tiles=tiles, head=head),
            out_shape=jax.ShapeDtypeStruct(
                (devices, batches * (rows + TERMS), HEAD), jnp.bfloat16
            ),
            in_specs=[
                smem,
                vmem,
                vmem,
                vmem,
            ],
            out_specs=vmem,
            scratch_shapes=[
                pltpu.VMEM((2, 2 * HEAD, 2 * rows), jnp.bfloat16),
                pltpu.VMEM((HEAD + 8, 2 * rows), jnp.float32),
                pltpu.VMEM((1, 2 * rows), jnp.float32),
            ],
            cost_estimate=pl.CostEstimate(flops=10**10, transcendentals=0, bytes_accessed=2**22),
            compiler_params=pltpu.CompilerParams(vmem_limit_bytes=GRANT),
            name="attend",
        )(slots, near(arrived[head]), close_keys, close_turned)
        returned.append(
            lax.all_to_all(partial, "seq", split_axis=0, concat_axis=0, tiled=True)
        )
    out = ()
    for head in range(shared):
        out = (
            pl.pallas_call(
                functools.partial(combine, tile_rows=tile_rows),
                out_shape=jax.ShapeDtypeStruct(
                    (batches, tile_rows, (head + 1) * width), jnp.bfloat16
                ),
                in_specs=[smem, smem, smem, vmem] + [vmem] * len(out),
                out_specs=vmem,
                cost_estimate=pl.CostEstimate(
                    flops=2 * 10**9, transcendentals=0, bytes_accessed=2**20
                ),
                compiler_params=pltpu.CompilerParams(vmem_limit_bytes=GRANT),
            name="combine",
            )(me, tile_blocks, block_place, near(returned[head]), *out),
        )
    return out[0][:, None]


def solution(mesh):
    placed = (
        P(None, ("groups", "seq"), None, "heads"),
        P(("groups", "seq"), None, "heads"),
        P(("groups", "seq"), None, "heads"),
        P("groups", None),
        P("groups"),
        P("groups"),
    )

    return jax.shard_map(
        local,
        mesh=mesh,
        in_specs=placed,
        out_specs=P(None, ("groups", "seq"), None, "heads"),
        check_vma=False,
    )
```

```python
import functools

import jax
import jax.numpy as jnp
from jax import lax
from jax.experimental import pallas as pl
from jax.experimental.pallas import tpu as pltpu
from jax.sharding import PartitionSpec as P


HEAD = 128
SCALE = HEAD ** (-0.5) * 1.4426950408889634
KEYS = 256
GRANT = 36 * 2**20
SMALL = 2.0**-60
LARGE = 2.0**100
TERMS = 4


def prepare(me, tile_blocks, block_place, tile_offset, values, turned, slots, *, tile_rows):
    keys, features = values.shape
    for head in range(features // HEAD):
        for start in range(0, keys, 512):
            turned[head, :, start : start + 512] = values[
                start : start + 512, head * HEAD : (head + 1) * HEAD
            ].T
    block_count = block_place.shape[0]
    tiles, top = tile_blocks.shape

    def find(block, mine):
        return jnp.where(block_place[block] == me[0], block, mine)

    mine = lax.fori_loop(0, block_count, find, 0)

    def visit(tile, counts, late):
        count = counts
        entries = [tile_blocks[tile, entry] for entry in range(top)]
        own = functools.reduce(jnp.maximum, entries) == mine
        named = functools.reduce(jnp.logical_or, [entry == mine for entry in entries])
        chosen = named & (own if late else jnp.logical_not(own))

        @pl.when(chosen)
        def _():
            slots[2 + count] = tile
            slots[3 + tiles + count] = tile_offset[tile] * tile_rows if late else keys

        return count + chosen.astype(jnp.int32)

    whole = lax.fori_loop(0, tiles, functools.partial(visit, late=False), 0)
    count = lax.fori_loop(0, tiles, functools.partial(visit, late=True), whole)
    slots[0] = whole // 2
    slots[1] = (count + 1) // 2

    @pl.when(count % 2 == 1)
    def _():
        slots[2 + count] = slots[1 + count]
        slots[3 + tiles + count] = slots[2 + tiles + count]


def attend(
    slots, queries, all_keys, both, partial, rotated, total, checks, turned, arrival, *, tiles, head
):
    devices, batches, tile_rows, width = queries.shape
    group = width // HEAD
    rows = tile_rows * group
    keys_ref = all_keys.at[:, head * HEAD : (head + 1) * HEAD]
    copy = pltpu.make_async_copy(both.at[head], turned, arrival)
    copy.start()
    key_count = all_keys.shape[0]
    columns = 2 * rows
    steps = key_count // (2 * KEYS)
    checks[...] = jnp.ones(checks.shape, jnp.float32)
    rotated[...] = jnp.zeros(rotated.shape, rotated.dtype)

    def tile_of(pair, side):
        tile = slots[2 + 2 * pair + side]
        return tile % devices, tile // devices

    def limits_of(pair):
        row = lax.broadcasted_iota(jnp.int32, (1, rows), 1) % tile_rows
        return jnp.concatenate(
            [slots[3 + tiles + 2 * pair + side] + row for side in range(2)], axis=1
        )

    def visible(start, limits):
        return lax.broadcasted_iota(jnp.int32, (KEYS, columns), 0) <= limits - start

    def load(pair, place):
        for side in range(2):
            device, batch = tile_of(pair, side)
            tile = queries[device, batch]
            stacked = jnp.concatenate(
                [tile[:, part * HEAD : (part + 1) * HEAD] for part in range(group)], axis=0
            )
            rotated[place, :HEAD, side * rows : (side + 1) * rows] = stacked.T

    def finish(pair, summed, highest):
        mass = jnp.log2(summed) + highest
        high = mass.astype(jnp.bfloat16)
        middle = (mass - high.astype(jnp.float32)).astype(jnp.bfloat16)
        low = (mass - high.astype(jnp.float32) - middle.astype(jnp.float32)).astype(jnp.bfloat16)
        pad = lax.broadcasted_iota(jnp.int32, (TERMS * batches, columns), 0)
        terms = jnp.where(
            pad % TERMS == 0,
            high.astype(jnp.float32),
            jnp.where(
                pad % TERMS == 1,
                middle.astype(jnp.float32),
                jnp.where(pad % TERMS == 2, low.astype(jnp.float32), 0.0),
            ),
        )
        blended = (total[:HEAD] * (1.0 / summed)).T.astype(jnp.bfloat16)
        for side in range(2):
            device, batch = tile_of(pair, side)
            part = slice(side * rows, (side + 1) * rows)
            partial[device, pl.ds(pl.multiple_of(batch * rows, rows), rows)] = blended[part]
            held = partial[device, batches * rows :].astype(jnp.float32)
            partial[device, batches * rows :] = jnp.where(
                pad[:, part] // TERMS == batch, terms[:, part], held
            ).astype(jnp.bfloat16)

    def quick(first, last, masked, accumulators):
        score = accumulators[:2], accumulators[2:4]
        value = accumulators[4:]

        def score_step(unit, place, step):
            start = (2 * step + unit) * KEYS
            block = keys_ref[start : start + KEYS]
            pltpu.matmul_push_rhs(rotated[place], 0, unit)
            pltpu.matmul_acc_lhs(
                score[unit][step % 2], jnp.concatenate([block, block], axis=1), 0
            )

        def value_step(unit, step, limits):
            start = (2 * step + unit) * KEYS
            weights = jnp.exp2(pltpu.matmul_pop(score[unit][step % 2]) * SCALE)
            if masked:
                weights = jnp.where(visible(start, limits), weights, 0.0)
            pltpu.matmul_push_rhs(weights.astype(jnp.bfloat16), 1, unit)
            pltpu.matmul_acc_lhs(value[unit], turned[:, start : start + KEYS], 1)
            return jnp.sum(weights.reshape(KEYS // 8, 8, columns), axis=0)

        def close(pair, real):
            total[:HEAD] = pltpu.matmul_pop(value[0]) + pltpu.matmul_pop(value[1])
            summed = jnp.sum(total[HEAD:], axis=0, keepdims=True)
            good = (summed > SMALL) & (summed < LARGE)
            checks[...] = jnp.minimum(checks[...], jnp.where(good | jnp.logical_not(real), 1.0, 0.0))
            finish(pair, summed, 0.0)

        for unit in range(2):
            for accumulator in score[unit] + value[unit : unit + 1]:
                pltpu.matmul_pop(accumulator)
        total[HEAD:] = jnp.ones((8, columns), jnp.float32)
        load(first, first % 2)
        for unit in range(2):
            score_step(unit, first % 2, 0)

        def body(pair, carry):
            place = pair % 2
            limits = limits_of(pair) if masked else None
            close(jnp.maximum(pair - 1, first), pair > first)
            load(jnp.minimum(pair + 1, last - 1), 1 - place)
            for step in range(steps):
                for unit in range(2):
                    if step + 1 < steps:
                        score_step(unit, place, step + 1)
                    else:
                        score_step(unit, 1 - place, 0)
                    added = value_step(unit, step, limits)
                    whole = added if step + unit == 0 else whole + added
            total[HEAD:] = whole
            return carry

        lax.fori_loop(first, last, body, 0)
        for unit in range(2):
            pltpu.matmul_pop(score[unit][0])
        close(last - 1, True)

    def exact(pair, carry, accumulators):
        score, value = accumulators[0], accumulators[4]
        load(pair, 0)
        limits = limits_of(pair)

        def measured(step):
            start = pl.multiple_of(step * KEYS, KEYS)
            block = keys_ref[pl.ds(start, KEYS), :]
            pltpu.matmul_push_rhs(rotated[0], 0, 0)
            pltpu.matmul_acc_lhs(score, jnp.concatenate([block, block], axis=1), 0)
            scores = pltpu.matmul_pop(score) * SCALE
            return jnp.where(visible(start, limits), scores, -1e30)

        def highest_of(step, highest):
            return jnp.maximum(highest, jnp.max(measured(step), axis=0, keepdims=True))

        highest = lax.fori_loop(
            0, key_count // KEYS, highest_of, jnp.full((1, columns), -1e30, jnp.float32)
        )

        def add(step, summed):
            weights = jnp.exp2(measured(step) - highest)
            pltpu.matmul_push_rhs(weights.astype(jnp.bfloat16), 1, 0)
            pltpu.matmul_acc_lhs(
                value, turned[:, pl.ds(pl.multiple_of(step * KEYS, KEYS), KEYS)], 1
            )
            return summed + jnp.sum(weights, axis=0, keepdims=True)

        summed = lax.fori_loop(
            0, key_count // KEYS, add, jnp.zeros((1, columns), jnp.float32)
        )
        total[:HEAD] = pltpu.matmul_pop(value)
        finish(pair, summed, highest)
        return carry

    def every(*accumulators):
        copy.wait()

        @pl.when(slots[0] > 0)
        def _():
            quick(0, slots[0], False, accumulators)

        @pl.when(slots[1] > slots[0])
        def _():
            quick(slots[0], slots[1], True, accumulators)

        @pl.when(jnp.min(checks[...]) < 0.5)
        def _():
            lax.fori_loop(
                0, slots[1], functools.partial(exact, accumulators=accumulators), 0
            )

    pl.run_scoped(
        every,
        *[pltpu.ACC(unit)((KEYS, columns), jnp.float32) for unit in (0, 0, 1, 1)],
        *[pltpu.ACC(unit)((HEAD, columns), jnp.float32) for unit in (0, 1)],
    )


def combine(me, tile_blocks, block_place, returned, *rest, tile_rows):
    *rest, attended = rest
    devices, padded, _ = returned.shape
    batches = attended.shape[0]
    top = tile_blocks.shape[1]
    rows = padded // batches - TERMS
    start = 0
    for earlier in rest:
        attended[:, :, : earlier.shape[2]] = earlier[...]
        start = earlier.shape[2]
    for batch in range(batches):
        owners = [
            block_place[tile_blocks[batch * devices + me[0], entry]] for entry in range(top)
        ]
        masses = []
        for owner in owners:
            terms = returned[owner, batches * rows :].astype(jnp.float32)
            first = batch * TERMS
            masses.append(
                terms[first : first + 1] + terms[first + 1 : first + 2] + terms[first + 2 : first + 3]
            )
        highest = functools.reduce(jnp.maximum, masses)
        shares = [jnp.exp2(mass - highest) for mass in masses]
        inverse = 1.0 / functools.reduce(jnp.add, shares)
        stacked = jnp.concatenate(
            [share * inverse for share in shares] + [jnp.zeros((8 - top, rows), jnp.float32)],
            axis=0,
        ).T
        blended = functools.reduce(
            jnp.add,
            [
                stacked[:, entry : entry + 1]
                * returned[owner, batch * rows : (batch + 1) * rows].astype(jnp.float32)
                for entry, owner in enumerate(owners)
            ],
        ).astype(jnp.bfloat16)
        for part in range(rows // tile_rows):
            column = start + part * HEAD
            attended[batch, :, column : column + HEAD] = blended[
                part * tile_rows : (part + 1) * tile_rows
            ]


def near(array):
    return pltpu.with_memory_space_constraint(array, pltpu.VMEM)


def local(queries, keys, values, tile_blocks, block_place, tile_offset):
    devices = lax.axis_size("seq")
    batches, _, tile_rows, features = queries.shape
    _, key_count, key_features = keys.shape
    shared = key_features // HEAD
    width = features // shared
    rows = tile_rows * (width // HEAD)
    tiles = tile_blocks.shape[0]
    me = lax.axis_index("seq").astype(jnp.int32)[None]
    smem = pl.BlockSpec(memory_space=pltpu.SMEM)
    vmem = pl.BlockSpec(memory_space=pltpu.VMEM)
    turned, slots = pl.pallas_call(
        functools.partial(prepare, tile_rows=tile_rows),
        out_shape=(
            jax.ShapeDtypeStruct((shared, HEAD, key_count), jnp.bfloat16),
            jax.ShapeDtypeStruct((2 * tiles + 5,), jnp.int32),
        ),
        in_specs=[smem, smem, smem, smem, vmem],
        out_specs=(vmem, smem),
        cost_estimate=pl.CostEstimate(flops=10**10, transcendentals=0, bytes_accessed=2**22),
        compiler_params=pltpu.CompilerParams(vmem_limit_bytes=GRANT),
            name="prepare",
    )(me, tile_blocks, block_place, tile_offset, values[0])
    arrived = []
    for head in range(shared):
        source = lax.optimization_barrier(queries) if head else queries
        tile = source[:, 0, :, head * width : (head + 1) * width]
        outgoing = jnp.broadcast_to(tile[None], (devices,) + tile.shape)
        arrived.append(
            lax.all_to_all(outgoing, "seq", split_axis=0, concat_axis=0, tiled=True)
        )
    close_keys = near(keys[0])
    turned = pltpu.with_memory_space_constraint(turned, pltpu.HBM)
    returned = []
    for head in range(shared):
        partial = pl.pallas_call(
            functools.partial(attend, tiles=tiles, head=head),
            out_shape=jax.ShapeDtypeStruct(
                (devices, batches * (rows + TERMS), HEAD), jnp.bfloat16
            ),
            in_specs=[
                smem,
                vmem,
                vmem,
                pl.BlockSpec(memory_space=pltpu.HBM),
            ],
            out_specs=vmem,
            scratch_shapes=[
                pltpu.VMEM((2, 2 * HEAD, 2 * rows), jnp.bfloat16),
                pltpu.VMEM((HEAD + 8, 2 * rows), jnp.float32),
                pltpu.VMEM((1, 2 * rows), jnp.float32),
                pltpu.VMEM((HEAD, key_count), jnp.bfloat16),
                pltpu.SemaphoreType.DMA,
            ],
            cost_estimate=pl.CostEstimate(flops=10**10, transcendentals=0, bytes_accessed=2**22),
            compiler_params=pltpu.CompilerParams(vmem_limit_bytes=GRANT),
            name="attend",
        )(slots, near(arrived[head]), close_keys, turned)
        returned.append(
            lax.all_to_all(partial, "seq", split_axis=0, concat_axis=0, tiled=True)
        )
    out = ()
    for head in range(shared):
        out = (
            pl.pallas_call(
                functools.partial(combine, tile_rows=tile_rows),
                out_shape=jax.ShapeDtypeStruct(
                    (batches, tile_rows, (head + 1) * width), jnp.bfloat16
                ),
                in_specs=[smem, smem, smem, vmem] + [vmem] * len(out),
                out_specs=vmem,
                cost_estimate=pl.CostEstimate(
                    flops=2 * 10**9, transcendentals=0, bytes_accessed=2**20
                ),
                compiler_params=pltpu.CompilerParams(vmem_limit_bytes=GRANT),
            name="combine",
            )(me, tile_blocks, block_place, near(returned[head]), *out),
        )
    return out[0][:, None]


def solution(mesh):
    placed = (
        P(None, ("groups", "seq"), None, "heads"),
        P(("groups", "seq"), None, "heads"),
        P(("groups", "seq"), None, "heads"),
        P("groups", None),
        P("groups"),
        P("groups"),
    )

    return jax.shard_map(
        local,
        mesh=mesh,
        in_specs=placed,
        out_specs=P(None, ("groups", "seq"), None, "heads"),
        check_vma=False,
    )
```

```python
import functools

import jax
import jax.numpy as jnp
from jax import lax
from jax.experimental import pallas as pl
from jax.experimental.pallas import tpu as pltpu
from jax.sharding import PartitionSpec as P


HEAD = 128
SCALE = HEAD ** (-0.5) * 1.4426950408889634
KEYS = 256
GRANT = 36 * 2**20
SMALL = 2.0**-60
LARGE = 2.0**100
TERMS = 4


def prepare(me, tile_blocks, block_place, tile_offset, values, turned, slots, *, tile_rows):
    keys, features = values.shape
    for head in range(features // HEAD):
        for start in range(0, keys, 512):
            turned[head, :, start : start + 512] = values[
                start : start + 512, head * HEAD : (head + 1) * HEAD
            ].T
    block_count = block_place.shape[0]
    tiles, top = tile_blocks.shape

    def find(block, mine):
        return jnp.where(block_place[block] == me[0], block, mine)

    mine = lax.fori_loop(0, block_count, find, 0)

    def visit(tile, count, kind):
        entries = [tile_blocks[tile, entry] for entry in range(top)]
        own = functools.reduce(jnp.maximum, entries) == mine
        named = functools.reduce(jnp.logical_or, [entry == mine for entry in entries])
        near = tile_offset[tile] * tile_rows + tile_rows <= keys // 2
        wanted = (jnp.logical_not(own), own & jnp.logical_not(near), own & near)
        chosen = named & wanted[kind]

        @pl.when(chosen)
        def _():
            slots[2 + count] = tile
            slots[3 + tiles + count] = tile_offset[tile] * tile_rows if kind else keys

        return count + chosen.astype(jnp.int32)

    whole = lax.fori_loop(0, tiles, functools.partial(visit, kind=0), 0)
    count = lax.fori_loop(0, tiles, functools.partial(visit, kind=1), whole)
    count = lax.fori_loop(0, tiles, functools.partial(visit, kind=2), count)
    slots[0] = whole // 2
    slots[1] = (count + 1) // 2

    @pl.when(count % 2 == 1)
    def _():
        slots[2 + count] = slots[1 + count]
        slots[3 + tiles + count] = slots[2 + tiles + count]


def attend(
    slots, queries, all_keys, both, partial, rotated, total, checks, turned, arrival, *, tiles, head
):
    devices, batches, tile_rows, width = queries.shape
    group = width // HEAD
    rows = tile_rows * group
    keys_ref = all_keys.at[:, head * HEAD : (head + 1) * HEAD]
    copy = pltpu.make_async_copy(both.at[head], turned, arrival)
    copy.start()
    key_count = all_keys.shape[0]
    columns = 2 * rows
    steps = key_count // (2 * KEYS)
    checks[...] = jnp.ones(checks.shape, jnp.float32)
    rotated[...] = jnp.zeros(rotated.shape, rotated.dtype)

    def tile_of(pair, side):
        tile = slots[2 + 2 * pair + side]
        return tile % devices, tile // devices

    def limits_of(pair):
        row = lax.broadcasted_iota(jnp.int32, (1, rows), 1) % tile_rows
        return jnp.concatenate(
            [slots[3 + tiles + 2 * pair + side] + row for side in range(2)], axis=1
        )

    def visible(start, limits):
        return lax.broadcasted_iota(jnp.int32, (KEYS, columns), 0) <= limits - start

    def load(pair, place):
        for side in range(2):
            device, batch = tile_of(pair, side)
            tile = queries[device, batch]
            stacked = jnp.concatenate(
                [tile[:, part * HEAD : (part + 1) * HEAD] for part in range(group)], axis=0
            )
            rotated[place, :HEAD, side * rows : (side + 1) * rows] = stacked.T

    def finish(pair, summed, highest):
        mass = jnp.log2(summed) + highest
        high = mass.astype(jnp.bfloat16)
        middle = (mass - high.astype(jnp.float32)).astype(jnp.bfloat16)
        low = (mass - high.astype(jnp.float32) - middle.astype(jnp.float32)).astype(jnp.bfloat16)
        pad = lax.broadcasted_iota(jnp.int32, (TERMS * batches, columns), 0)
        terms = jnp.where(
            pad % TERMS == 0,
            high.astype(jnp.float32),
            jnp.where(
                pad % TERMS == 1,
                middle.astype(jnp.float32),
                jnp.where(pad % TERMS == 2, low.astype(jnp.float32), 0.0),
            ),
        )
        blended = (total[:HEAD] * (1.0 / summed)).T.astype(jnp.bfloat16)
        for side in range(2):
            device, batch = tile_of(pair, side)
            part = slice(side * rows, (side + 1) * rows)
            partial[device, pl.ds(pl.multiple_of(batch * rows, rows), rows)] = blended[part]
            held = partial[device, batches * rows :].astype(jnp.float32)
            partial[device, batches * rows :] = jnp.where(
                pad[:, part] // TERMS == batch, terms[:, part], held
            ).astype(jnp.bfloat16)

    def quick(first, last, masked, accumulators):
        score = accumulators[:2], accumulators[2:4]
        value = accumulators[4:]

        def score_step(unit, place, step):
            start = (2 * step + unit) * KEYS
            block = keys_ref[start : start + KEYS]
            pltpu.matmul_push_rhs(rotated[place], 0, unit)
            pltpu.matmul_acc_lhs(
                score[unit][step % 2], jnp.concatenate([block, block], axis=1), 0
            )

        def value_step(unit, step, limits):
            start = (2 * step + unit) * KEYS
            weights = jnp.exp2(pltpu.matmul_pop(score[unit][step % 2]) * SCALE)
            if masked:
                weights = jnp.where(visible(start, limits), weights, 0.0)
            pltpu.matmul_push_rhs(weights.astype(jnp.bfloat16), 1, unit)
            pltpu.matmul_acc_lhs(value[unit], turned[:, start : start + KEYS], 1)
            return jnp.sum(weights.reshape(KEYS // 8, 8, columns), axis=0)

        def close(pair, real):
            total[:HEAD] = pltpu.matmul_pop(value[0]) + pltpu.matmul_pop(value[1])
            summed = jnp.sum(total[HEAD:], axis=0, keepdims=True)
            good = (summed > SMALL) & (summed < LARGE)
            checks[...] = jnp.minimum(checks[...], jnp.where(good | jnp.logical_not(real), 1.0, 0.0))
            finish(pair, summed, 0.0)

        for unit in range(2):
            for accumulator in score[unit] + value[unit : unit + 1]:
                pltpu.matmul_pop(accumulator)
        total[HEAD:] = jnp.ones((8, columns), jnp.float32)
        load(first, first % 2)
        for unit in range(2):
            score_step(unit, first % 2, 0)

        def body(pair, carry):
            place = pair % 2
            limits = limits_of(pair) if masked else None
            close(jnp.maximum(pair - 1, first), pair > first)
            load(jnp.minimum(pair + 1, last - 1), 1 - place)

            def advance(start, stop):
                added = []
                for step in range(start, stop):
                    for unit in range(2):
                        if step + 1 < steps:
                            score_step(unit, place, step + 1)
                        else:
                            score_step(unit, 1 - place, 0)
                        added.append(value_step(unit, step, limits))
                return functools.reduce(jnp.add, added)

            if not masked:
                total[HEAD:] = advance(0, steps)
                return carry
            total[HEAD:] = advance(0, steps // 2)
            farthest = functools.reduce(
                jnp.maximum, [slots[3 + tiles + 2 * pair + side] for side in range(2)]
            )
            beyond = farthest + tile_rows > key_count // 2

            @pl.when(beyond)
            def _():
                total[HEAD:] += advance(steps // 2, steps)

            @pl.when(jnp.logical_not(beyond))
            def _():
                for unit in range(2):
                    pltpu.matmul_pop(score[unit][steps // 2 % 2])
                    score_step(unit, 1 - place, 0)

            return carry

        lax.fori_loop(first, last, body, 0)
        for unit in range(2):
            pltpu.matmul_pop(score[unit][0])
        close(last - 1, True)

    def exact(pair, carry, accumulators):
        score, value = accumulators[0], accumulators[4]
        load(pair, 0)
        limits = limits_of(pair)

        def measured(step):
            start = pl.multiple_of(step * KEYS, KEYS)
            block = keys_ref[pl.ds(start, KEYS), :]
            pltpu.matmul_push_rhs(rotated[0], 0, 0)
            pltpu.matmul_acc_lhs(score, jnp.concatenate([block, block], axis=1), 0)
            scores = pltpu.matmul_pop(score) * SCALE
            return jnp.where(visible(start, limits), scores, -1e30)

        def highest_of(step, highest):
            return jnp.maximum(highest, jnp.max(measured(step), axis=0, keepdims=True))

        highest = lax.fori_loop(
            0, key_count // KEYS, highest_of, jnp.full((1, columns), -1e30, jnp.float32)
        )

        def add(step, summed):
            weights = jnp.exp2(measured(step) - highest)
            pltpu.matmul_push_rhs(weights.astype(jnp.bfloat16), 1, 0)
            pltpu.matmul_acc_lhs(
                value, turned[:, pl.ds(pl.multiple_of(step * KEYS, KEYS), KEYS)], 1
            )
            return summed + jnp.sum(weights, axis=0, keepdims=True)

        summed = lax.fori_loop(
            0, key_count // KEYS, add, jnp.zeros((1, columns), jnp.float32)
        )
        total[:HEAD] = pltpu.matmul_pop(value)
        finish(pair, summed, highest)
        return carry

    def every(*accumulators):
        copy.wait()

        @pl.when(slots[0] > 0)
        def _():
            quick(0, slots[0], False, accumulators)

        @pl.when(slots[1] > slots[0])
        def _():
            quick(slots[0], slots[1], True, accumulators)

        @pl.when(jnp.min(checks[...]) < 0.5)
        def _():
            lax.fori_loop(
                0, slots[1], functools.partial(exact, accumulators=accumulators), 0
            )

    pl.run_scoped(
        every,
        *[pltpu.ACC(unit)((KEYS, columns), jnp.float32) for unit in (0, 0, 1, 1)],
        *[pltpu.ACC(unit)((HEAD, columns), jnp.float32) for unit in (0, 1)],
    )


def combine(me, tile_blocks, block_place, returned, *rest, tile_rows):
    *rest, attended = rest
    devices, padded, _ = returned.shape
    batches = attended.shape[0]
    top = tile_blocks.shape[1]
    rows = padded // batches - TERMS
    start = 0
    for earlier in rest:
        attended[:, :, : earlier.shape[2]] = earlier[...]
        start = earlier.shape[2]
    for batch in range(batches):
        owners = [
            block_place[tile_blocks[batch * devices + me[0], entry]] for entry in range(top)
        ]
        masses = []
        for owner in owners:
            terms = returned[owner, batches * rows :].astype(jnp.float32)
            first = batch * TERMS
            masses.append(
                terms[first : first + 1] + terms[first + 1 : first + 2] + terms[first + 2 : first + 3]
            )
        highest = functools.reduce(jnp.maximum, masses)
        shares = [jnp.exp2(mass - highest) for mass in masses]
        inverse = 1.0 / functools.reduce(jnp.add, shares)
        stacked = jnp.concatenate(
            [share * inverse for share in shares] + [jnp.zeros((8 - top, rows), jnp.float32)],
            axis=0,
        ).T
        blended = functools.reduce(
            jnp.add,
            [
                stacked[:, entry : entry + 1]
                * returned[owner, batch * rows : (batch + 1) * rows].astype(jnp.float32)
                for entry, owner in enumerate(owners)
            ],
        ).astype(jnp.bfloat16)
        for part in range(rows // tile_rows):
            column = start + part * HEAD
            attended[batch, :, column : column + HEAD] = blended[
                part * tile_rows : (part + 1) * tile_rows
            ]


def near(array):
    return pltpu.with_memory_space_constraint(array, pltpu.VMEM)


def local(queries, keys, values, tile_blocks, block_place, tile_offset):
    devices = lax.axis_size("seq")
    batches, _, tile_rows, features = queries.shape
    _, key_count, key_features = keys.shape
    shared = key_features // HEAD
    width = features // shared
    rows = tile_rows * (width // HEAD)
    tiles = tile_blocks.shape[0]
    me = lax.axis_index("seq").astype(jnp.int32)[None]
    smem = pl.BlockSpec(memory_space=pltpu.SMEM)
    vmem = pl.BlockSpec(memory_space=pltpu.VMEM)
    turned, slots = pl.pallas_call(
        functools.partial(prepare, tile_rows=tile_rows),
        out_shape=(
            jax.ShapeDtypeStruct((shared, HEAD, key_count), jnp.bfloat16),
            jax.ShapeDtypeStruct((2 * tiles + 5,), jnp.int32),
        ),
        in_specs=[smem, smem, smem, smem, vmem],
        out_specs=(vmem, smem),
        cost_estimate=pl.CostEstimate(flops=10**10, transcendentals=0, bytes_accessed=2**22),
        compiler_params=pltpu.CompilerParams(vmem_limit_bytes=GRANT),
            name="prepare",
    )(me, tile_blocks, block_place, tile_offset, values[0])
    arrived = []
    for head in range(shared):
        source = lax.optimization_barrier(queries) if head else queries
        tile = source[:, 0, :, head * width : (head + 1) * width]
        outgoing = jnp.broadcast_to(tile[None], (devices,) + tile.shape)
        arrived.append(
            lax.all_to_all(outgoing, "seq", split_axis=0, concat_axis=0, tiled=True)
        )
    close_keys = near(keys[0])
    turned = pltpu.with_memory_space_constraint(turned, pltpu.HBM)
    returned = []
    for head in range(shared):
        partial = pl.pallas_call(
            functools.partial(attend, tiles=tiles, head=head),
            out_shape=jax.ShapeDtypeStruct(
                (devices, batches * (rows + TERMS), HEAD), jnp.bfloat16
            ),
            in_specs=[
                smem,
                vmem,
                vmem,
                pl.BlockSpec(memory_space=pltpu.HBM),
            ],
            out_specs=vmem,
            scratch_shapes=[
                pltpu.VMEM((2, 2 * HEAD, 2 * rows), jnp.bfloat16),
                pltpu.VMEM((HEAD + 8, 2 * rows), jnp.float32),
                pltpu.VMEM((1, 2 * rows), jnp.float32),
                pltpu.VMEM((HEAD, key_count), jnp.bfloat16),
                pltpu.SemaphoreType.DMA,
            ],
            cost_estimate=pl.CostEstimate(flops=10**10, transcendentals=0, bytes_accessed=2**22),
            compiler_params=pltpu.CompilerParams(vmem_limit_bytes=GRANT),
            name="attend",
        )(slots, near(arrived[head]), close_keys, turned)
        returned.append(
            lax.all_to_all(partial, "seq", split_axis=0, concat_axis=0, tiled=True)
        )
    out = ()
    for head in range(shared):
        out = (
            pl.pallas_call(
                functools.partial(combine, tile_rows=tile_rows),
                out_shape=jax.ShapeDtypeStruct(
                    (batches, tile_rows, (head + 1) * width), jnp.bfloat16
                ),
                in_specs=[smem, smem, smem, vmem] + [vmem] * len(out),
                out_specs=vmem,
                cost_estimate=pl.CostEstimate(
                    flops=2 * 10**9, transcendentals=0, bytes_accessed=2**20
                ),
                compiler_params=pltpu.CompilerParams(vmem_limit_bytes=GRANT),
            name="combine",
            )(me, tile_blocks, block_place, near(returned[head]), *out),
        )
    return out[0][:, None]


def solution(mesh):
    placed = (
        P(None, ("groups", "seq"), None, "heads"),
        P(("groups", "seq"), None, "heads"),
        P(("groups", "seq"), None, "heads"),
        P("groups", None),
        P("groups"),
        P("groups"),
    )

    return jax.shard_map(
        local,
        mesh=mesh,
        in_specs=placed,
        out_specs=P(None, ("groups", "seq"), None, "heads"),
        check_vma=False,
    )
```

```python
import functools

import jax
import jax.numpy as jnp
from jax import lax
from jax.experimental import pallas as pl
from jax.experimental.pallas import tpu as pltpu
from jax.sharding import PartitionSpec as P


HEAD = 128
SCALE = HEAD ** (-0.5) * 1.4426950408889634
KEYS = 256
GRANT = 36 * 2**20
SMALL = 2.0**-60
LARGE = 2.0**100
TERMS = 4


def prepare(me, tile_blocks, block_place, tile_offset, values, turned, slots, *, tile_rows):
    keys, features = values.shape
    for head in range(features // HEAD):
        for start in range(0, keys, 512):
            turned[head, :, start : start + 512] = values[
                start : start + 512, head * HEAD : (head + 1) * HEAD
            ].T
    block_count = block_place.shape[0]
    tiles, top = tile_blocks.shape

    def find(block, mine):
        return jnp.where(block_place[block] == me[0], block, mine)

    mine = lax.fori_loop(0, block_count, find, 0)

    def visit(tile, count, kind):
        entries = [tile_blocks[tile, entry] for entry in range(top)]
        own = functools.reduce(jnp.maximum, entries) == mine
        named = functools.reduce(jnp.logical_or, [entry == mine for entry in entries])
        near = tile_offset[tile] * tile_rows + tile_rows <= keys // 2
        wanted = (jnp.logical_not(own), own & jnp.logical_not(near), own & near)
        chosen = named & wanted[kind]

        @pl.when(chosen)
        def _():
            slots[2 + count] = tile
            slots[3 + tiles + count] = tile_offset[tile] * tile_rows if kind else keys

        return count + chosen.astype(jnp.int32)

    whole = lax.fori_loop(0, tiles, functools.partial(visit, kind=0), 0)
    count = lax.fori_loop(0, tiles, functools.partial(visit, kind=1), whole)
    count = lax.fori_loop(0, tiles, functools.partial(visit, kind=2), count)
    slots[0] = whole // 2
    slots[1] = (count + 1) // 2

    @pl.when(count % 2 == 1)
    def _():
        slots[2 + count] = slots[1 + count]
        slots[3 + tiles + count] = slots[2 + tiles + count]


def attend(
    slots, queries, all_keys, both, partial, rotated, total, checks, turned, arrival, *, tiles, head
):
    devices, batches, tile_rows, width = queries.shape
    group = width // HEAD
    rows = tile_rows * group
    keys_ref = all_keys.at[:, head * HEAD : (head + 1) * HEAD]
    copy = pltpu.make_async_copy(both.at[head], turned, arrival)
    copy.start()
    key_count = all_keys.shape[0]
    columns = 2 * rows
    steps = key_count // (2 * KEYS)
    checks[...] = jnp.ones(checks.shape, jnp.float32)
    rotated[...] = jnp.zeros(rotated.shape, rotated.dtype)

    def tile_of(pair, side):
        tile = slots[2 + 2 * pair + side]
        return tile % devices, tile // devices

    def limits_of(pair):
        row = lax.broadcasted_iota(jnp.int32, (1, rows), 1) % tile_rows
        return jnp.concatenate(
            [slots[3 + tiles + 2 * pair + side] + row for side in range(2)], axis=1
        )

    def visible(start, limits):
        return lax.broadcasted_iota(jnp.int32, (KEYS, columns), 0) <= limits - start

    def load(pair, place):
        for side in range(2):
            device, batch = tile_of(pair, side)
            tile = queries[device, batch]
            stacked = jnp.concatenate(
                [tile[:, part * HEAD : (part + 1) * HEAD] for part in range(group)], axis=0
            )
            rotated[place, :HEAD, side * rows : (side + 1) * rows] = stacked.T

    def finish(pair, summed, highest):
        mass = jnp.log2(summed) + highest
        high = mass.astype(jnp.bfloat16)
        middle = (mass - high.astype(jnp.float32)).astype(jnp.bfloat16)
        low = (mass - high.astype(jnp.float32) - middle.astype(jnp.float32)).astype(jnp.bfloat16)
        pad = lax.broadcasted_iota(jnp.int32, (TERMS * batches, columns), 0)
        terms = jnp.where(
            pad % TERMS == 0,
            high.astype(jnp.float32),
            jnp.where(
                pad % TERMS == 1,
                middle.astype(jnp.float32),
                jnp.where(pad % TERMS == 2, low.astype(jnp.float32), 0.0),
            ),
        )
        blended = (total[:HEAD] * (1.0 / summed)).T.astype(jnp.bfloat16)
        for side in range(2):
            device, batch = tile_of(pair, side)
            part = slice(side * rows, (side + 1) * rows)
            partial[device, pl.ds(pl.multiple_of(batch * rows, rows), rows)] = blended[part]
            held = partial[device, batches * rows :].astype(jnp.float32)
            partial[device, batches * rows :] = jnp.where(
                pad[:, part] // TERMS == batch, terms[:, part], held
            ).astype(jnp.bfloat16)

    def quick(first, last, masked, accumulators):
        score = accumulators[:2], accumulators[2:4]
        value = accumulators[4:]

        def score_step(unit, place, step):
            start = (2 * step + unit) * KEYS
            block = keys_ref[start : start + KEYS]
            pltpu.matmul_push_rhs(rotated[place], 0, unit)
            pltpu.matmul_acc_lhs(
                score[unit][step % 2], jnp.concatenate([block, block], axis=1), 0
            )

        def value_step(unit, step, limits):
            start = (2 * step + unit) * KEYS
            weights = jnp.exp2(pltpu.matmul_pop(score[unit][step % 2]) * SCALE)
            if masked:
                weights = jnp.where(visible(start, limits), weights, 0.0)
            pltpu.matmul_push_rhs(weights.astype(jnp.bfloat16), 1, unit)
            pltpu.matmul_acc_lhs(value[unit], turned[:, start : start + KEYS], 1)
            return jnp.sum(weights.reshape(KEYS // 8, 8, columns), axis=0)

        def close(pair, real):
            total[:HEAD] = pltpu.matmul_pop(value[0]) + pltpu.matmul_pop(value[1])
            summed = jnp.sum(total[HEAD:], axis=0, keepdims=True)
            good = (summed > SMALL) & (summed < LARGE)
            checks[...] = jnp.minimum(checks[...], jnp.where(good | jnp.logical_not(real), 1.0, 0.0))
            finish(pair, summed, 0.0)

        for unit in range(2):
            for accumulator in score[unit] + value[unit : unit + 1]:
                pltpu.matmul_pop(accumulator)
        total[HEAD:] = jnp.ones((8, columns), jnp.float32)
        load(first, first % 2)
        for unit in range(2):
            score_step(unit, first % 2, 0)

        @pl.when(first == 0)
        def _():
            copy.wait()

        def body(pair, carry):
            place = pair % 2
            limits = limits_of(pair) if masked else None
            close(jnp.maximum(pair - 1, first), pair > first)
            load(jnp.minimum(pair + 1, last - 1), 1 - place)

            def advance(start, stop):
                added = []
                for step in range(start, stop):
                    for unit in range(2):
                        if step + 1 < steps:
                            score_step(unit, place, step + 1)
                        else:
                            score_step(unit, 1 - place, 0)
                        added.append(value_step(unit, step, limits))
                return functools.reduce(jnp.add, added)

            if not masked:
                total[HEAD:] = advance(0, steps)
                return carry
            total[HEAD:] = advance(0, steps // 2)
            farthest = functools.reduce(
                jnp.maximum, [slots[3 + tiles + 2 * pair + side] for side in range(2)]
            )
            beyond = farthest + tile_rows > key_count // 2

            @pl.when(beyond)
            def _():
                total[HEAD:] += advance(steps // 2, steps)

            @pl.when(jnp.logical_not(beyond))
            def _():
                for unit in range(2):
                    pltpu.matmul_pop(score[unit][steps // 2 % 2])
                    score_step(unit, 1 - place, 0)

            return carry

        lax.fori_loop(first, last, body, 0)
        for unit in range(2):
            pltpu.matmul_pop(score[unit][0])
        close(last - 1, True)

    def exact(pair, carry, accumulators):
        score, value = accumulators[0], accumulators[4]
        load(pair, 0)
        limits = limits_of(pair)

        def measured(step):
            start = pl.multiple_of(step * KEYS, KEYS)
            block = keys_ref[pl.ds(start, KEYS), :]
            pltpu.matmul_push_rhs(rotated[0], 0, 0)
            pltpu.matmul_acc_lhs(score, jnp.concatenate([block, block], axis=1), 0)
            scores = pltpu.matmul_pop(score) * SCALE
            return jnp.where(visible(start, limits), scores, -1e30)

        def highest_of(step, highest):
            return jnp.maximum(highest, jnp.max(measured(step), axis=0, keepdims=True))

        highest = lax.fori_loop(
            0, key_count // KEYS, highest_of, jnp.full((1, columns), -1e30, jnp.float32)
        )

        def add(step, summed):
            weights = jnp.exp2(measured(step) - highest)
            pltpu.matmul_push_rhs(weights.astype(jnp.bfloat16), 1, 0)
            pltpu.matmul_acc_lhs(
                value, turned[:, pl.ds(pl.multiple_of(step * KEYS, KEYS), KEYS)], 1
            )
            return summed + jnp.sum(weights, axis=0, keepdims=True)

        summed = lax.fori_loop(
            0, key_count // KEYS, add, jnp.zeros((1, columns), jnp.float32)
        )
        total[:HEAD] = pltpu.matmul_pop(value)
        finish(pair, summed, highest)
        return carry

    def every(*accumulators):
        @pl.when(slots[1] == 0)
        def _():
            copy.wait()

        @pl.when(slots[0] > 0)
        def _():
            quick(0, slots[0], False, accumulators)

        @pl.when(slots[1] > slots[0])
        def _():
            quick(slots[0], slots[1], True, accumulators)

        @pl.when(jnp.min(checks[...]) < 0.5)
        def _():
            lax.fori_loop(
                0, slots[1], functools.partial(exact, accumulators=accumulators), 0
            )

    pl.run_scoped(
        every,
        *[pltpu.ACC(unit)((KEYS, columns), jnp.float32) for unit in (0, 0, 1, 1)],
        *[pltpu.ACC(unit)((HEAD, columns), jnp.float32) for unit in (0, 1)],
    )


def combine(me, tile_blocks, block_place, returned, *rest, tile_rows):
    *rest, attended = rest
    devices, padded, _ = returned.shape
    batches = attended.shape[0]
    top = tile_blocks.shape[1]
    rows = padded // batches - TERMS
    start = 0
    for earlier in rest:
        attended[:, :, : earlier.shape[2]] = earlier[...]
        start = earlier.shape[2]
    for batch in range(batches):
        owners = [
            block_place[tile_blocks[batch * devices + me[0], entry]] for entry in range(top)
        ]
        masses = []
        for owner in owners:
            terms = returned[owner, batches * rows :].astype(jnp.float32)
            first = batch * TERMS
            masses.append(
                terms[first : first + 1] + terms[first + 1 : first + 2] + terms[first + 2 : first + 3]
            )
        highest = functools.reduce(jnp.maximum, masses)
        shares = [jnp.exp2(mass - highest) for mass in masses]
        inverse = 1.0 / functools.reduce(jnp.add, shares)
        stacked = jnp.concatenate(
            [share * inverse for share in shares] + [jnp.zeros((8 - top, rows), jnp.float32)],
            axis=0,
        ).T
        blended = functools.reduce(
            jnp.add,
            [
                stacked[:, entry : entry + 1]
                * returned[owner, batch * rows : (batch + 1) * rows].astype(jnp.float32)
                for entry, owner in enumerate(owners)
            ],
        ).astype(jnp.bfloat16)
        for part in range(rows // tile_rows):
            column = start + part * HEAD
            attended[batch, :, column : column + HEAD] = blended[
                part * tile_rows : (part + 1) * tile_rows
            ]


def near(array):
    return pltpu.with_memory_space_constraint(array, pltpu.VMEM)


def local(queries, keys, values, tile_blocks, block_place, tile_offset):
    devices = lax.axis_size("seq")
    batches, _, tile_rows, features = queries.shape
    _, key_count, key_features = keys.shape
    shared = key_features // HEAD
    width = features // shared
    rows = tile_rows * (width // HEAD)
    tiles = tile_blocks.shape[0]
    me = lax.axis_index("seq").astype(jnp.int32)[None]
    smem = pl.BlockSpec(memory_space=pltpu.SMEM)
    vmem = pl.BlockSpec(memory_space=pltpu.VMEM)
    turned, slots = pl.pallas_call(
        functools.partial(prepare, tile_rows=tile_rows),
        out_shape=(
            jax.ShapeDtypeStruct((shared, HEAD, key_count), jnp.bfloat16),
            jax.ShapeDtypeStruct((2 * tiles + 5,), jnp.int32),
        ),
        in_specs=[smem, smem, smem, smem, vmem],
        out_specs=(vmem, smem),
        cost_estimate=pl.CostEstimate(flops=10**10, transcendentals=0, bytes_accessed=2**22),
        compiler_params=pltpu.CompilerParams(vmem_limit_bytes=GRANT),
            name="prepare",
    )(me, tile_blocks, block_place, tile_offset, values[0])
    arrived = []
    for head in range(shared):
        source = lax.optimization_barrier(queries) if head else queries
        tile = source[:, 0, :, head * width : (head + 1) * width]
        outgoing = jnp.broadcast_to(tile[None], (devices,) + tile.shape)
        arrived.append(
            lax.all_to_all(outgoing, "seq", split_axis=0, concat_axis=0, tiled=True)
        )
    close_keys = near(keys[0])
    turned = pltpu.with_memory_space_constraint(turned, pltpu.HBM)
    returned = []
    for head in range(shared):
        partial = pl.pallas_call(
            functools.partial(attend, tiles=tiles, head=head),
            out_shape=jax.ShapeDtypeStruct(
                (devices, batches * (rows + TERMS), HEAD), jnp.bfloat16
            ),
            in_specs=[
                smem,
                vmem,
                vmem,
                pl.BlockSpec(memory_space=pltpu.HBM),
            ],
            out_specs=vmem,
            scratch_shapes=[
                pltpu.VMEM((2, 2 * HEAD, 2 * rows), jnp.bfloat16),
                pltpu.VMEM((HEAD + 8, 2 * rows), jnp.float32),
                pltpu.VMEM((1, 2 * rows), jnp.float32),
                pltpu.VMEM((HEAD, key_count), jnp.bfloat16),
                pltpu.SemaphoreType.DMA,
            ],
            cost_estimate=pl.CostEstimate(flops=10**10, transcendentals=0, bytes_accessed=2**22),
            compiler_params=pltpu.CompilerParams(vmem_limit_bytes=GRANT),
            name="attend",
        )(slots, near(arrived[head]), close_keys, turned)
        returned.append(
            lax.all_to_all(partial, "seq", split_axis=0, concat_axis=0, tiled=True)
        )
    out = ()
    for head in range(shared):
        out = (
            pl.pallas_call(
                functools.partial(combine, tile_rows=tile_rows),
                out_shape=jax.ShapeDtypeStruct(
                    (batches, tile_rows, (head + 1) * width), jnp.bfloat16
                ),
                in_specs=[smem, smem, smem, vmem] + [vmem] * len(out),
                out_specs=vmem,
                cost_estimate=pl.CostEstimate(
                    flops=2 * 10**9, transcendentals=0, bytes_accessed=2**20
                ),
                compiler_params=pltpu.CompilerParams(vmem_limit_bytes=GRANT),
            name="combine",
            )(me, tile_blocks, block_place, near(returned[head]), *out),
        )
    return out[0][:, None]


def solution(mesh):
    placed = (
        P(None, ("groups", "seq"), None, "heads"),
        P(("groups", "seq"), None, "heads"),
        P(("groups", "seq"), None, "heads"),
        P("groups", None),
        P("groups"),
        P("groups"),
    )

    return jax.shard_map(
        local,
        mesh=mesh,
        in_specs=placed,
        out_specs=P(None, ("groups", "seq"), None, "heads"),
        check_vma=False,
    )
```
